512 devices in a mesh: grid: 64 (over z, y_hi, x), band: 8 (over y_lo, core).
Axes of the slice: x: 4, y: 8 (y_hi: 2, y_lo: 4; y = y_hi * 4 + y_lo), z: 8, core: 2. Of those that a mesh axis runs over, the one named last changes fastest.
Arguments:
- states: float32 [16384, 1024], P('grid', 'band'), may hold values from -6 to 6
- potential: float32 [16384], P('grid'), may hold values from -3 to 0
- bounds: float32 [3], replicated, may hold values from -9 to 26, as said below
- point_count: int32 [64], P('grid'), may hold values from 128 to 256, as said below
- send_rows: int32 [64, 6, 64], P('grid'), may hold values from 0 to 256, as said below
- stencil_table: int32 [36, 16384], P(None, 'grid'), may hold values from 0 to 640, as said below
Outputs:
- filtered: float32 [16384, 1024], P('grid', 'band')
- margin: float32 [1024, 1024], P(('grid', 'band'))
The draws below stay inside these ranges and needn't reach their ends.
Inputs may be any that keep to these rules, and one draw needn't show every extreme that they name: `point_count`: one partition has exactly 256 live points in every draw; rows at or past a partition's count are padding. send_rows[g, k, j] is the row of partition g sent as row j of its block to partition g + o_k (o_k as in the reference program). A block has a length from half of 64 to 64: below it the entries are live rows of g, from it on they are 256; some block is full in every draw. Blocks to partitions that do not exist hold only 256. stencil_table[s, g * 256 + r] indexes E_g: values below 256 are live rows of partition g, 256 is the zero row, 257 + k * 64 + j is row j of the block from partition g - o_k, named only when that partition exists. Padding rows hold only 256; rows r below 160 name no block. bounds holds lower, cutoff and upper in this order: lower between -9 and -5, cutoff between -1.5 and 1.5, upper between 21 and 26.
All inputs are finite; a program needn't handle non-finite values.
Results may differ from the reference program's by a relative error of at most 0.0018.
Values may be sent and summed in bfloat16 or wider, within the bound.
No kernel may reach another device: no remote copies, remote signals or barrier semaphores. Data moves between devices by JAX's collectives and lax.ppermute only.
A program may use at most 64 MiB of HBM per device.

```python
import jax
import jax.numpy as jnp
from jax import lax

P_DEV = 256
HALO = 64
REACH = 3
SPAN = 6
DEGREE = 3
STENCIL = 36
INNER = 160
POINTS = 16384
BANDS = 1024
N_GRID = 64


def partition_sizes(key):
    sizes = jax.random.randint(jax.random.fold_in(key, 11), (N_GRID,), P_DEV // 2, P_DEV + 1)
    fullest = jax.random.randint(jax.random.fold_in(key, 12), (), 0, N_GRID)
    return jnp.where(jnp.arange(N_GRID) == fullest, P_DEV, sizes).astype(jnp.int32)


def slot_offsets():
    slots = jnp.arange(2 * REACH)
    return jnp.where(slots < REACH, slots - REACH, slots - REACH + 1)


def draw_point_count(key, part):
    return partition_sizes(key)


def draw_send_rows(key, part):
    sizes = partition_sizes(key)
    lengths = jax.random.randint(jax.random.fold_in(key, 21), (N_GRID, 2 * REACH), HALO // 2, HALO + 1)
    full_source = jax.random.randint(jax.random.fold_in(key, 22), (), 0, N_GRID - REACH)
    full_slot = jax.random.randint(jax.random.fold_in(key, 23), (), REACH, 2 * REACH)
    partitions = jnp.arange(N_GRID)[:, None]
    slots = jnp.arange(2 * REACH)[None, :]
    lengths = jnp.where(jnp.logical_and(partitions == full_source, slots == full_slot), HALO, lengths)
    target = partitions + slot_offsets()[None, :]
    exists = jnp.logical_and(target >= 0, target < N_GRID)
    picks = jax.random.randint(jax.random.fold_in(key, 24), (N_GRID, 2 * REACH, HALO), 0, 1 << 30) % sizes[:, None, None]
    positions = jnp.arange(HALO)[None, None, :]
    used = jnp.logical_and(positions < lengths[:, :, None], exists[:, :, None])
    return jnp.where(used, picks, P_DEV).astype(jnp.int32)


def draw_stencil_table(key, part):
    sizes = partition_sizes(key)
    shaped = (STENCIL, N_GRID, P_DEV)
    kinds = jax.random.randint(jax.random.fold_in(key, 31), shaped, 0, 20)
    local_pick = jax.random.randint(jax.random.fold_in(key, 32), shaped, 0, 1 << 30) % sizes[None, :, None]
    ghost_slot = jax.random.randint(jax.random.fold_in(key, 33), shaped, 0, 2 * REACH)
    ghost_row = jax.random.randint(jax.random.fold_in(key, 34), shaped, 0, HALO)
    partitions = jnp.arange(N_GRID)[None, :, None]
    source = partitions - slot_offsets()[ghost_slot]
    exists = jnp.logical_and(source >= 0, source < N_GRID)
    row_index = jnp.arange(P_DEV)[None, None, :]
    ghost_index = P_DEV + 1 + ghost_slot * HALO + ghost_row
    use_ghost = jnp.logical_and(jnp.logical_and(kinds >= 14, kinds < 19), row_index >= INNER)
    chosen = jnp.where(jnp.logical_and(use_ghost, exists), ghost_index, local_pick)
    chosen = jnp.where(jnp.logical_and(use_ghost, jnp.logical_not(exists)), P_DEV, chosen)
    chosen = jnp.where(jnp.logical_or(kinds >= 19, row_index >= sizes[None, :, None]), P_DEV, chosen)
    return chosen.reshape(STENCIL, N_GRID * P_DEV).astype(jnp.int32)


def draw_bounds(key, part):
    lower_bound = jax.random.uniform(jax.random.fold_in(key, 41), (), jnp.float32, -8.0, -6.0)
    cutoff = jax.random.uniform(jax.random.fold_in(key, 42), (), jnp.float32, -1.0, 1.0)
    upper_bound = jax.random.uniform(jax.random.fold_in(key, 43), (), jnp.float32, 22.0, 25.0)
    return jnp.stack([lower_bound, cutoff, upper_bound]).astype(jnp.float32)


def level_of(stream_key, extent, shards, low, largest):
    loudness, own = 1.0, jax.random.fold_in(stream_key, 6)
    for axis_at, blocks in shards:
        steps = jnp.exp(jax.random.uniform(jax.random.fold_in(own, axis_at), (blocks,), jnp.float32, low / len(shards), largest / len(shards)))
        loudness = loudness * jnp.repeat(steps, extent[axis_at] // blocks).reshape([-1 if axis == axis_at else 1 for axis in range(len(extent))])
    return loudness


def scatter_about(stream_key, extent, scale, limit, shards=(), held_as=jnp.bfloat16):
    gain = level_of(stream_key, extent, shards, -0.22, 0.18) if shards else 1.0
    values = jax.random.normal(stream_key, extent, jnp.float32) * scale * gain
    return jnp.minimum(jnp.maximum(values, -limit), limit).astype(held_as)


def setup_inputs(seed: int = 0) -> dict:
    streams_of = jax.random.split(jax.random.key(seed), 7)
    states = scatter_about(streams_of[0], (POINTS, BANDS), 1.0, 6.0, ((0, 64), (1, 8)), jnp.float32)
    potential = jnp.clip(-3.0 + 3.0 * jax.random.uniform(streams_of[1], (POINTS,), jnp.float32) ** level_of(streams_of[1], (POINTS,), ((0, 64),), -0.2, 0.2), -3.0, 0.0)
    bounds = draw_bounds(jax.random.fold_in(streams_of[6], 71), 0)
    point_count = draw_point_count(jax.random.fold_in(streams_of[6], 71), 0)
    send_rows = draw_send_rows(jax.random.fold_in(streams_of[6], 71), 0)
    stencil_table = draw_stencil_table(jax.random.fold_in(streams_of[6], 71), 0)
    return {"states": states, "potential": potential, "bounds": bounds, "point_count": point_count, "send_rows": send_rows, "stencil_table": stencil_table}


DIFFERENCE_WEIGHTS = (-5369.0 / 1800.0, 12.0 / 7.0, -15.0 / 56.0, 10.0 / 189.0, -1.0 / 112.0, 2.0 / 1925.0, -1.0 / 16632.0)
KINETIC_SCALE = 0.5 / 0.49
CENTRE_WEIGHT = -3.0 * KINETIC_SCALE * DIFFERENCE_WEIGHTS[0]


def apply_stencil(extended, local_table, fields, potentials):
    result = (potentials + CENTRE_WEIGHT)[:, None] * fields
    for neighbour in range(local_table.shape[0]):
        weight = -KINETIC_SCALE * DIFFERENCE_WEIGHTS[neighbour % SPAN + 1]
        result = result + weight * jnp.take(extended, local_table[neighbour], axis=0)
    return result


def apply_operator(fields, potentials, send_rows, stencil_table):
    grid_count, row_count, band_total = fields.shape
    half_slots = send_rows.shape[1] // 2
    zero_row = jnp.zeros((1, band_total), jnp.float32)

    def partition_image(partition):
        pieces = [fields[partition], zero_row]
        for slot_index in range(2 * half_slots):
            offset = slot_index - half_slots if slot_index < half_slots else slot_index - half_slots + 1
            source = partition - offset
            inside = jnp.logical_and(source >= 0, source < grid_count)
            clipped = jnp.clip(source, 0, grid_count - 1)
            source_rows = jnp.concatenate([fields[clipped], zero_row], axis=0)
            outgoing = jnp.take(source_rows, send_rows[clipped, slot_index], axis=0)
            pieces.append(jnp.where(inside, outgoing, 0.0))
        extended = jnp.concatenate(pieces, axis=0)
        local_table = lax.dynamic_slice_in_dim(stencil_table, partition * row_count, row_count, 1)
        return apply_stencil(extended, local_table, fields[partition], potentials[partition])

    return lax.map(partition_image, jnp.arange(grid_count, dtype=jnp.int32))


def reference(states, potential, bounds, point_count, send_rows, stencil_table):
    fields = states.reshape(N_GRID, P_DEV, BANDS)
    potentials = potential.reshape(N_GRID, P_DEV)
    live_rows = jnp.arange(P_DEV, dtype=jnp.int32)[None, :] < point_count[:, None]
    previous = jnp.where(live_rows[:, :, None], fields, 0.0)
    lower_bound = bounds[0]
    cutoff = bounds[1]
    upper_bound = bounds[2]
    half_width = (upper_bound - cutoff) / 2.0
    middle = (upper_bound + cutoff) / 2.0
    sigma_now = half_width / (lower_bound - middle)
    twice_inverse = 2.0 / sigma_now
    applied = apply_operator(previous, potentials, send_rows, stencil_table)
    current = (applied - middle * previous) * (sigma_now / half_width)
    for degree_index in range(DEGREE - 1):
        sigma_next = 1.0 / (twice_inverse - sigma_now)
        applied = apply_operator(current, potentials, send_rows, stencil_table)
        following = (applied - middle * current) * (2.0 * sigma_next / half_width) - (sigma_now * sigma_next) * previous
        previous = current
        current = following
        sigma_now = sigma_next
    filtered = current.reshape(POINTS, BANDS)
    rounded = filtered.astype(jnp.bfloat16)
    margin = jnp.dot(rounded.T, rounded, preferred_element_type=jnp.float32) * (1.0 / POINTS)
    return filtered, margin
```

```python
import functools

import jax
import jax.numpy as jnp
from jax import lax
from jax.experimental import pallas as pl
from jax.experimental.pallas import tpu as pltpu
from jax.sharding import PartitionSpec as P

SPAN = 6
DEGREE = 3
REACH = 3
GROUP = 8

DIFFERENCE_WEIGHTS = (
    -5369.0 / 1800.0,
    12.0 / 7.0,
    -15.0 / 56.0,
    10.0 / 189.0,
    -1.0 / 112.0,
    2.0 / 1925.0,
    -1.0 / 16632.0,
)
KINETIC_SCALE = 0.5 / 0.49
CENTRE_WEIGHT = -3.0 * KINETIC_SCALE * DIFFERENCE_WEIGHTS[0]
TILE = 128
BF16 = jnp.bfloat16
F32 = jnp.float32
VMEM = pl.BlockSpec(memory_space=pltpu.VMEM)
SMEM = pl.BlockSpec(memory_space=pltpu.SMEM)


def dot(a, b):
    return jnp.dot(a, b, preferred_element_type=F32)


def split(values):
    high = values.astype(BF16)
    return high, (values - high.astype(F32)).astype(BF16)


def select_rows(select_ref, sends_ref, first, blocks, rows):
    for pair in range((blocks + 1) // 2):
        picks = sends_ref[pl.ds(first + 2 * pair, 1), :]
        height = min(TILE, 64 * (blocks - 2 * pair))
        for at in range(0, rows, TILE):
            here = lax.broadcasted_iota(jnp.int32, (TILE, TILE), 0) + at
            hit = jnp.where(here == picks, 1.0, 0.0)
            select_ref[pl.ds(pair * TILE, height), pl.ds(at, TILE)] = jnp.transpose(hit)[:height].astype(BF16)


def begin_kernel(place_ref, count_ref, sends_ref, states_ref, start_ref, own_ref, cross_ref, crossing_ref):
    place = place_ref[0]
    rows = states_ref.shape[0]
    live = lax.broadcasted_iota(jnp.int32, states_ref.shape, 0) < count_ref[0]
    start = jnp.where(live, states_ref[...], 0.0)
    start_ref[...] = start
    first = jnp.where(place >= 5, 15 - place, jnp.maximum(4 - place, 0))
    select_rows(cross_ref, sends_ref, first, REACH, rows)
    crossing_ref[...] = dot(cross_ref[...], start.astype(BF16)).astype(BF16)
    select_rows(own_ref, sends_ref, 7 - place, GROUP, rows)


def local_part(fields, high_ref, low_ref, own_ref, part_ref, outgoing_ref):
    high, low = split(fields)
    part_ref[...] = dot(high_ref[...], high) + dot(low_ref[...], high) + dot(high_ref[...], low)
    outgoing_ref[...] = dot(own_ref[...], high).astype(BF16)


def build_kernel(
    place_ref, bounds_ref, potential_ref, table_ref, start_ref, own_ref,
    high_ref, low_ref, halo_high_ref, halo_low_ref, part_ref, outgoing_ref, halo_table
):
    place = place_ref[0]
    rows = start_ref.shape[0]
    stencil = table_ref.shape[0]
    middle = (bounds_ref[2] + bounds_ref[1]) / 2.0
    table = table_ref[...]
    slot = jnp.right_shift(table - (rows + 1), 6)
    offset = slot - jnp.where(slot < REACH, REACH, REACH - 1)
    source = jnp.bitwise_and(place - offset, GROUP - 1)
    halo = source * 64 + jnp.bitwise_and(table - (rows + 1), 63)
    halo_table[...] = jnp.where(table > rows, halo, -1)

    def gathered(names_ref, column, row):
        here = lax.broadcasted_iota(jnp.int32, (TILE, TILE), 0) + column
        total = jnp.zeros((TILE, TILE), F32)
        for neighbour in range(stencil):
            weight = -KINETIC_SCALE * DIFFERENCE_WEIGHTS[neighbour % SPAN + 1]
            names = names_ref[neighbour : neighbour + 1, row : row + TILE]
            total = total + jnp.where(here == names, weight, 0.0)
        return total, here

    for row in range(0, rows, TILE):
        diagonal = potential_ref[:, row : row + TILE] + (CENTRE_WEIGHT - middle)

        @pl.loop(0, rows // TILE)
        def _(block, row=row, diagonal=diagonal):
            column = pl.multiple_of(block * TILE, TILE)
            total, here = gathered(table_ref, column, row)
            right = lax.broadcasted_iota(jnp.int32, (TILE, TILE), 1) + row
            total = total + jnp.where(here == right, diagonal, 0.0)
            high, low = split(jnp.transpose(total))
            high_ref[pl.ds(row, TILE), pl.ds(column, TILE)] = high
            low_ref[pl.ds(row, TILE), pl.ds(column, TILE)] = low

    @pl.loop(0, GROUP * 64 // TILE)
    def _(block):
        column = pl.multiple_of(block * TILE, TILE)
        total, _ = gathered(halo_table, column, rows - TILE)
        high, low = split(jnp.transpose(total))
        halo_high_ref[:, pl.ds(column, TILE)] = high
        halo_low_ref[:, pl.ds(column, TILE)] = low

    local_part(start_ref[...], high_ref, low_ref, own_ref, part_ref, outgoing_ref)


def local_kernel(fields_ref, high_ref, low_ref, own_ref, part_ref, outgoing_ref):
    local_part(fields_ref[...], high_ref, low_ref, own_ref, part_ref, outgoing_ref)


def update_kernel(degree, bounds_ref, part_ref, halo_ref, halo_high_ref, halo_low_ref, *rest):
    refs = list(rest)
    before_ref = refs.pop(0) if degree > 0 else None
    cross_ref = refs.pop(0) if degree < DEGREE - 1 else None
    fields_ref, extra_ref = refs
    spread = lambda at: jnp.full((8, TILE), bounds_ref[at], F32)
    lower, cutoff, upper = spread(0), spread(1), spread(2)
    half = (upper - cutoff) / 2.0
    middle = (upper + cutoff) / 2.0
    sigma = half / (lower - middle)
    twice = 2.0 / sigma
    scale, carried = sigma / half, None
    for _ in range(degree):
        following = 1.0 / (twice - sigma)
        scale, carried = 2.0 * following / half, sigma * following
        sigma = following
    rows = part_ref.shape[0]
    halo = halo_ref[...]
    reached = dot(halo_high_ref[...], halo) + dot(halo_low_ref[...], halo)
    for at in range(0, rows, TILE):
        image = part_ref[pl.ds(at, TILE), :]
        if at == rows - TILE:
            image = image + reached
        image = image * scale[:1]
        if degree > 0:
            image = image - carried[:1] * before_ref[pl.ds(at, TILE), :]
        fields_ref[pl.ds(at, TILE), :] = image
        if degree == DEGREE - 1:
            extra_ref[pl.ds(at, TILE), :] = image.astype(BF16)
    if degree < DEGREE - 1:
        extra_ref[...] = dot(cross_ref[...], fields_ref[...].astype(BF16)).astype(BF16)


def margin_kernel(band_ref, every_ref, partial_ref):
    bands, _, width = every_ref.shape
    wanted = 2 * bands
    row = lax.broadcasted_iota(jnp.int32, (wanted, width), 0)
    column = lax.broadcasted_iota(jnp.int32, (wanted, width), 1)
    target = jnp.right_shift(row, 1) * wanted + 2 * band_ref[0] + jnp.bitwise_and(row, 1)
    pick = jnp.where(column == target, 1.0, 0.0).astype(BF16)
    chosen = [
        lax.dot_general(pick, every_ref[band], (((1,), (1,)), ((), ())), preferred_element_type=F32).astype(BF16)
        for band in range(bands)
    ]
    chosen = jnp.concatenate(chosen, axis=0)
    for band in range(bands):
        partial_ref[:, pl.ds(band * width, width)] = dot(chosen, every_ref[band]).astype(BF16)


def call(kernel, operands, specs, outs, flops, scratch=()):
    moved = sum(x.size * x.dtype.itemsize for x in (*operands, *outs))
    return pl.pallas_call(
        kernel,
        out_shape=tuple(outs),
        in_specs=specs,
        out_specs=tuple(VMEM for _ in outs),
        scratch_shapes=list(scratch),
        compiler_params=pltpu.CompilerParams(vmem_limit_bytes=16 * 1024 * 1024),
        cost_estimate=pl.CostEstimate(flops=flops, bytes_accessed=moved, transcendentals=0),
    )(*operands)


def shape(dims, dtype=F32):
    return jax.ShapeDtypeStruct(dims, dtype)


def across(crossing, parts):
    route = []
    for at in range(parts):
        place = at % GROUP
        if place >= 5 and at + GROUP < parts:
            route.append((at, at + GROUP))
        if place <= 2 and at >= GROUP:
            route.append((at, at - GROUP))
    return lax.ppermute(crossing, "grid", route)


def exchanged(outgoing, relayed, place, parts):
    zeros = jnp.zeros_like(relayed)
    down = jnp.where(place >= 5, relayed, zeros)
    up = jnp.where(place <= 2, relayed, zeros)
    gap = jnp.zeros((outgoing.shape[0] - 2 * relayed.shape[0], relayed.shape[1]), BF16)
    message = (outgoing + jnp.concatenate([down, gap, up], axis=0)).reshape(GROUP, -1, outgoing.shape[1])
    groups = [list(range(first, first + GROUP)) for first in range(0, parts, GROUP)]
    received = lax.all_to_all(message, "grid", 0, 0, axis_index_groups=groups, tiled=True)
    return received.reshape(outgoing.shape)


def on_device(states, potential, bounds, point_count, send_rows, stencil_table):
    rows, width = states.shape
    stencil = stencil_table.shape[0]
    parts = lax.axis_size("grid")
    bands = lax.axis_size("band")
    slots = GROUP * 64
    place = lax.rem(lax.axis_index("grid"), GROUP).reshape(1)
    none = jnp.full((4, 64), rows, jnp.int32)
    lined = jnp.concatenate([none, send_rows[0, :REACH], none[:1], send_rows[0, REACH:], none, none[:1]], axis=0)
    paired = jnp.concatenate([lined, jnp.concatenate([lined[1:], none[:1]], axis=0)], axis=1)

    start, own, cross, crossing = call(
        begin_kernel,
        (place, point_count, paired, states),
        [SMEM, SMEM, VMEM, VMEM],
        [shape((rows, width)), shape((slots, rows), BF16), shape((REACH * 64, rows), BF16), shape((REACH * 64, width), BF16)],
        10_000_000,
    )
    relayed = across(crossing, parts)
    high, low, halo_high, halo_low, part, outgoing = call(
        build_kernel,
        (place, bounds, potential.reshape(1, rows), stencil_table, start, own),
        [SMEM, SMEM, VMEM, VMEM, VMEM, VMEM],
        [
            shape((rows, rows), BF16),
            shape((rows, rows), BF16),
            shape((TILE, slots), BF16),
            shape((TILE, slots), BF16),
            shape((rows, width)),
            shape((slots, width), BF16),
        ],
        50_000_000,
        [pltpu.VMEM((stencil, rows), jnp.int32)],
    )
    before, fields = None, start
    for degree in range(DEGREE):
        if degree > 0:
            relayed = across(extra, parts)
            part, outgoing = call(
                local_kernel,
                (fields, high, low, own),
                [VMEM] * 4,
                [shape((rows, width)), shape((slots, width), BF16)],
                80_000_000,
            )
        halo = exchanged(outgoing, relayed, place[0], parts)
        operands = [bounds, part, halo, halo_high, halo_low]
        if degree > 0:
            operands.append(before)
        if degree < DEGREE - 1:
            operands.append(cross)
            after = shape((REACH * 64, width), BF16)
        else:
            after = shape((rows, width), BF16)
        before = fields
        fields, extra = call(
            functools.partial(update_kernel, degree),
            operands,
            [SMEM] + [VMEM] * (len(operands) - 1),
            [shape((rows, width)), after],
            40_000_000,
        )
    every_band = lax.all_gather(extra, "band", axis=0)
    (partial_sums,) = call(
        margin_kernel,
        (lax.axis_index("band").reshape(1), every_band),
        [SMEM, VMEM],
        [shape((2 * parts, bands * width), BF16)],
        80_000_000,
    )
    blocks = lax.all_to_all(partial_sums.reshape(parts, 2, bands * width), "grid", 0, 0, tiled=True)
    summed = jnp.sum(blocks.astype(F32), axis=0)
    return fields, summed * (1.0 / (parts * rows))


def solution(mesh):
    placed = (P("grid", "band"), P("grid"), P(), P("grid"), P("grid", None, None), P(None, "grid"))
    return jax.shard_map(
        on_device,
        mesh=mesh,
        in_specs=placed,
        out_specs=(P("grid", "band"), P(("grid", "band"), None)),
        check_vma=False,
    )
```

```python
import functools

import jax
import jax.numpy as jnp
from jax import lax
from jax.experimental import pallas as pl
from jax.experimental.pallas import tpu as pltpu
from jax.sharding import PartitionSpec as P

SPAN = 6
DEGREE = 3
REACH = 3
GROUP = 8

DIFFERENCE_WEIGHTS = (
    -5369.0 / 1800.0,
    12.0 / 7.0,
    -15.0 / 56.0,
    10.0 / 189.0,
    -1.0 / 112.0,
    2.0 / 1925.0,
    -1.0 / 16632.0,
)
KINETIC_SCALE = 0.5 / 0.49
CENTRE_WEIGHT = -3.0 * KINETIC_SCALE * DIFFERENCE_WEIGHTS[0]
TILE = 128
BF16 = jnp.bfloat16
F32 = jnp.float32
VMEM = pl.BlockSpec(memory_space=pltpu.VMEM)
SMEM = pl.BlockSpec(memory_space=pltpu.SMEM)


def dot(a, b):
    return jnp.dot(a, b, preferred_element_type=F32)


def split(values):
    high = values.astype(BF16)
    return high, (values - high.astype(F32)).astype(BF16)


def select_rows(select_ref, sends_ref, offsets, rows):
    def block(offset):
        picks = jnp.full((1, 64), rows, jnp.int32)
        for slot in range(2 * REACH):
            kept = slot - REACH if slot < REACH else slot - REACH + 1
            picks = jnp.where(offset == kept, sends_ref[slot], picks)
        return picks

    for pair in range((len(offsets) + 1) // 2):
        two = [block(offset) for offset in offsets[2 * pair : 2 * pair + 2]]
        height = 64 * len(two)
        picks = jnp.concatenate([two[0], two[-1]], axis=1)
        for at in range(0, rows, TILE):
            here = lax.broadcasted_iota(jnp.int32, (TILE, TILE), 0) + at
            hit = jnp.where(here == picks, 1.0, 0.0)
            select_ref[pl.ds(pair * TILE, height), pl.ds(at, TILE)] = jnp.transpose(hit)[:height].astype(BF16)


def begin_kernel(
    place_ref, band_ref, count_ref, sends_ref, states_ref, start_ref, own_ref, cross_ref, crossing_ref
):
    place = place_ref[0]
    rows = states_ref.shape[0]
    first = jnp.where(place >= 5, GROUP - place, -REACH - place)
    select_rows(cross_ref, sends_ref, [first + at for at in range(REACH)], rows)
    live = lax.broadcasted_iota(jnp.int32, states_ref.shape, 0) < count_ref[0]
    start = jnp.where(live, states_ref[...], 0.0)
    start_ref[...] = start
    crossing_ref[...] = dot(cross_ref[...], start.astype(BF16)).astype(BF16)
    select_rows(own_ref, sends_ref, [at - place for at in range(GROUP)], rows)


def local_part(fields, high_ref, low_ref, own_ref, part_ref, outgoing_ref):
    high, low = split(fields)
    part_ref[...] = dot(high_ref[...], high) + dot(low_ref[...], high) + dot(high_ref[...], low)
    outgoing_ref[...] = dot(own_ref[...], high).astype(BF16)


def build_kernel(
    place_ref, bounds_ref, potential_ref, table_ref, start_ref, own_ref,
    high_ref, low_ref, halos_ref, factors_ref, part_ref, outgoing_ref, halo_table
):
    place = place_ref[0]
    rows = start_ref.shape[0]
    stencil = table_ref.shape[0]
    lower, cutoff, upper = (jnp.broadcast_to(bounds_ref[:, at : at + 1], (8, TILE)) for at in range(3))
    half = (upper - cutoff) / 2.0
    middle = (upper + cutoff) / 2.0
    sigma = half / (lower - middle)
    twice = 2.0 / sigma
    factors_ref[0] = sigma / half
    factors_ref[1] = jnp.zeros_like(sigma)
    for degree in range(1, DEGREE):
        following = 1.0 / (twice - sigma)
        factors_ref[2 * degree] = 2.0 * following / half
        factors_ref[2 * degree + 1] = sigma * following
        sigma = following
    middle = middle[:1]
    table = table_ref[...]
    slot = jnp.right_shift(table - (rows + 1), 6)
    offset = slot - jnp.where(slot < REACH, REACH, REACH - 1)
    source = jnp.bitwise_and(place - offset, GROUP - 1)
    halo = source * 64 + jnp.bitwise_and(table - (rows + 1), 63)
    halo_table[...] = jnp.where(table > rows, halo, -1)

    def gathered(names_ref, column, row):
        here = lax.broadcasted_iota(jnp.int32, (TILE, TILE), 0) + column
        total = jnp.zeros((TILE, TILE), F32)
        for neighbour in range(stencil):
            weight = -KINETIC_SCALE * DIFFERENCE_WEIGHTS[neighbour % SPAN + 1]
            names = names_ref[neighbour : neighbour + 1, row : row + TILE]
            total = total + jnp.where(here == names, weight, 0.0)
        return total, here

    for row in range(0, rows, TILE):
        diagonal = potential_ref[:, row : row + TILE] + (CENTRE_WEIGHT - middle)

        @pl.loop(0, rows // TILE)
        def _(block, row=row, diagonal=diagonal):
            column = pl.multiple_of(block * TILE, TILE)
            total, here = gathered(table_ref, column, row)
            right = lax.broadcasted_iota(jnp.int32, (TILE, TILE), 1) + row
            total = total + jnp.where(here == right, diagonal, 0.0)
            high, low = split(jnp.transpose(total))
            high_ref[pl.ds(row, TILE), pl.ds(column, TILE)] = high
            low_ref[pl.ds(row, TILE), pl.ds(column, TILE)] = low

    @pl.loop(0, GROUP * 64 // TILE)
    def _(block):
        column = pl.multiple_of(block * TILE, TILE)
        total, _ = gathered(halo_table, column, rows - TILE)
        high, low = split(jnp.transpose(total))
        halos_ref[pl.ds(0, TILE), pl.ds(column, TILE)] = high
        halos_ref[pl.ds(TILE, TILE), pl.ds(column, TILE)] = low

    local_part(start_ref[...], high_ref, low_ref, own_ref, part_ref, outgoing_ref)


def local_kernel(fields_ref, high_ref, low_ref, own_ref, part_ref, outgoing_ref):
    local_part(fields_ref[...], high_ref, low_ref, own_ref, part_ref, outgoing_ref)


def update_kernel(degree, factors_ref, part_ref, halo_ref, halos_ref, *rest):
    refs = list(rest)
    before_ref = refs.pop(0) if degree > 0 else None
    cross_ref = refs.pop(0) if degree < DEGREE - 1 else None
    fields_ref, extra_ref = refs
    scale = factors_ref[2 * degree][:1]
    carried = factors_ref[2 * degree + 1][:1]
    rows = part_ref.shape[0]
    reached = dot(halos_ref[...], halo_ref[...])
    reached = reached[:TILE] + reached[TILE:]
    for at in range(0, rows, TILE):
        image = part_ref[pl.ds(at, TILE), :]
        if at == rows - TILE:
            image = image + reached
        image = image * scale
        if degree > 0:
            image = image - carried * before_ref[pl.ds(at, TILE), :]
        fields_ref[pl.ds(at, TILE), :] = image
        if degree == DEGREE - 1:
            extra_ref[pl.ds(at, TILE), :] = image.astype(BF16)
    if degree < DEGREE - 1:
        extra_ref[...] = dot(cross_ref[...], fields_ref[...].astype(BF16)).astype(BF16)


def end_kernel(scaling, fields_ref, summed_ref, filtered_ref, margin_ref):
    filtered_ref[...] = fields_ref[...]
    margin_ref[...] = summed_ref[...] * scaling


def margin_kernel(band_ref, every_ref, partial_ref):
    bands, _, width = every_ref.shape
    wanted = 2 * bands
    row = lax.broadcasted_iota(jnp.int32, (wanted, width), 0)
    column = lax.broadcasted_iota(jnp.int32, (wanted, width), 1)
    target = jnp.right_shift(row, 1) * wanted + 2 * band_ref[0] + jnp.bitwise_and(row, 1)
    pick = jnp.where(column == target, 1.0, 0.0).astype(BF16)
    chosen = [
        lax.dot_general(pick, every_ref[band], (((1,), (1,)), ((), ())), preferred_element_type=F32).astype(BF16)
        for band in range(bands)
    ]
    chosen = jnp.concatenate(chosen, axis=0)
    for band in range(bands):
        partial_ref[:, pl.ds(band * width, width)] = dot(chosen, every_ref[band]).astype(BF16)


def call(kernel, operands, specs, outs, flops, scratch=()):
    moved = sum(x.size * x.dtype.itemsize for x in (*operands, *outs))
    return pl.pallas_call(
        kernel,
        out_shape=tuple(outs),
        in_specs=specs,
        out_specs=tuple(VMEM for _ in outs),
        scratch_shapes=list(scratch),
        compiler_params=pltpu.CompilerParams(vmem_limit_bytes=16 * 1024 * 1024),
        cost_estimate=pl.CostEstimate(flops=flops, bytes_accessed=moved, transcendentals=0),
    )(*operands)


def shape(dims, dtype=F32):
    return jax.ShapeDtypeStruct(dims, dtype)


def across(crossing, parts):
    route = []
    for at in range(parts):
        place = at % GROUP
        if place >= 5 and at + GROUP < parts:
            route.append((at, at + GROUP))
        if place <= 2 and at >= GROUP:
            route.append((at, at - GROUP))
    return lax.ppermute(crossing, "grid", route)


def exchanged(outgoing, relayed, place, parts):
    zeros = jnp.zeros_like(relayed)
    down = jnp.where(place >= 5, relayed, zeros)
    up = jnp.where(place <= 2, relayed, zeros)
    gap = jnp.zeros((outgoing.shape[0] - 2 * relayed.shape[0], relayed.shape[1]), BF16)
    message = (outgoing + jnp.concatenate([down, gap, up], axis=0)).reshape(GROUP, -1, outgoing.shape[1])
    groups = [list(range(first, first + GROUP)) for first in range(0, parts, GROUP)]
    received = lax.all_to_all(message, "grid", 0, 0, axis_index_groups=groups, tiled=True)
    return received.reshape(outgoing.shape)


def on_device(states, potential, bounds, point_count, send_rows, stencil_table):
    rows, width = states.shape
    stencil = stencil_table.shape[0]
    parts = lax.axis_size("grid")
    bands = lax.axis_size("band")
    slots = GROUP * 64
    place = jnp.bitwise_and(lax.axis_index("grid"), GROUP - 1).reshape(1)
    band = lax.axis_index("band").reshape(1)

    start, own, cross, crossing = call(
        begin_kernel,
        (place, band, point_count, jnp.swapaxes(send_rows, 0, 1), states),
        [SMEM, SMEM, SMEM, VMEM, VMEM],
        [shape((rows, width)), shape((slots, rows), BF16), shape((REACH * 64, rows), BF16), shape((REACH * 64, width), BF16)],
        10_000_000,
    )
    relayed = across(crossing, parts)
    high, low, halos, factors, part, outgoing = call(
        build_kernel,
        (place, bounds.reshape(1, 3), potential.reshape(1, rows), stencil_table, start, own),
        [SMEM, VMEM, VMEM, VMEM, VMEM, VMEM],
        [
            shape((rows, rows), BF16),
            shape((rows, rows), BF16),
            shape((2 * TILE, slots), BF16),
            shape((2 * DEGREE, 8, TILE)),
            shape((rows, width)),
            shape((slots, width), BF16),
        ],
        50_000_000,
        [pltpu.VMEM((stencil, rows), jnp.int32)],
    )
    before, fields = None, start
    for degree in range(DEGREE):
        if degree > 0:
            relayed = across(extra, parts)
            part, outgoing = call(
                local_kernel,
                (fields, high, low, own),
                [VMEM] * 4,
                [shape((rows, width)), shape((slots, width), BF16)],
                80_000_000,
            )
        halo = exchanged(outgoing, relayed, place[0], parts)
        operands = [factors, part, halo, halos]
        if degree > 0:
            operands.append(before)
        if degree < DEGREE - 1:
            operands.append(cross)
            after = shape((REACH * 64, width), BF16)
        else:
            after = shape((rows, width), BF16)
        before = fields
        fields, extra = call(
            functools.partial(update_kernel, degree),
            operands,
            [VMEM] * len(operands),
            [shape((rows, width)), after],
            40_000_000,
        )
    every_band = lax.all_gather(extra, "band", axis=0)
    (partial_sums,) = call(
        margin_kernel,
        (band, every_band),
        [SMEM, VMEM],
        [shape((2 * parts, bands * width), BF16)],
        80_000_000,
    )
    blocks = lax.all_to_all(partial_sums.reshape(parts, 2, bands * width), "grid", 0, 0, tiled=True)
    summed = jnp.sum(blocks.astype(F32), axis=0)
    return call(
        functools.partial(end_kernel, 1.0 / (parts * rows)),
        (fields, summed),
        [VMEM, VMEM],
        [shape((rows, width)), shape(summed.shape)],
        1000,
    )


def solution(mesh):
    placed = (P("grid", "band"), P("grid"), P(), P("grid"), P("grid", None, None), P(None, "grid"))
    return jax.shard_map(
        on_device,
        mesh=mesh,
        in_specs=placed,
        out_specs=(P("grid", "band"), P(("grid", "band"), None)),
        check_vma=False,
    )
```

```python
import functools

import jax
import jax.numpy as jnp
from jax import lax
from jax.experimental import pallas as pl
from jax.experimental.pallas import tpu as pltpu
from jax.sharding import PartitionSpec as P

SPAN = 6
DEGREE = 3
REACH = 3
GROUP = 8

DIFFERENCE_WEIGHTS = (
    -5369.0 / 1800.0,
    12.0 / 7.0,
    -15.0 / 56.0,
    10.0 / 189.0,
    -1.0 / 112.0,
    2.0 / 1925.0,
    -1.0 / 16632.0,
)
KINETIC_SCALE = 0.5 / 0.49
CENTRE_WEIGHT = -3.0 * KINETIC_SCALE * DIFFERENCE_WEIGHTS[0]
TILE = 128
BF16 = jnp.bfloat16
F32 = jnp.float32
VMEM = pl.BlockSpec(memory_space=pltpu.VMEM)
SMEM = pl.BlockSpec(memory_space=pltpu.SMEM)


def dot(a, b):
    return jnp.dot(a, b, preferred_element_type=F32)


def split(values):
    high = values.astype(BF16)
    return high, (values - high.astype(F32)).astype(BF16)


def select_rows(select_ref, sends_ref, offsets, rows):
    def block(offset):
        picks = jnp.full((1, 64), rows, jnp.int32)
        for slot in range(2 * REACH):
            kept = slot - REACH if slot < REACH else slot - REACH + 1
            picks = jnp.where(offset == kept, sends_ref[slot], picks)
        return picks

    for pair in range((len(offsets) + 1) // 2):
        two = [block(offset) for offset in offsets[2 * pair : 2 * pair + 2]]
        height = 64 * len(two)
        picks = jnp.concatenate([two[0], two[-1]], axis=1)
        for at in range(0, rows, TILE):
            here = lax.broadcasted_iota(jnp.int32, (TILE, TILE), 0) + at
            hit = jnp.where(here == picks, 1.0, 0.0)
            select_ref[pl.ds(pair * TILE, height), pl.ds(at, TILE)] = jnp.transpose(hit)[:height].astype(BF16)


def begin_kernel(
    place_ref, band_ref, count_ref, sends_ref, states_ref, start_ref, own_ref, cross_ref, crossing_ref
):
    place = place_ref[0]
    rows = states_ref.shape[0]
    first = jnp.where(place >= 5, GROUP - place, -REACH - place)
    select_rows(cross_ref, sends_ref, [first + at for at in range(REACH)], rows)
    live = lax.broadcasted_iota(jnp.int32, states_ref.shape, 0) < count_ref[0]
    start = jnp.where(live, states_ref[...], 0.0)
    start_ref[...] = start
    crossing_ref[...] = dot(cross_ref[...], start.astype(BF16)).astype(BF16)
    select_rows(own_ref, sends_ref, [at - place for at in range(GROUP)], rows)


def local_part(fields, high_ref, low_ref, own_ref, part_ref, outgoing_ref):
    high, low = split(fields)
    part_ref[...] = dot(high_ref[...], high) + dot(low_ref[...], high) + dot(high_ref[...], low)
    outgoing_ref[...] = dot(own_ref[...], high).astype(BF16)


def build_kernel(
    place_ref, bounds_ref, potential_ref, table_ref, start_ref, own_ref,
    high_ref, low_ref, halos_ref, factors_ref, part_ref, outgoing_ref, halo_table
):
    place = place_ref[0]
    rows = start_ref.shape[0]
    stencil = table_ref.shape[0]
    lower, cutoff, upper = (jnp.broadcast_to(bounds_ref[:, at : at + 1], (8, TILE)) for at in range(3))
    half = (upper - cutoff) / 2.0
    middle = (upper + cutoff) / 2.0
    sigma = half / (lower - middle)
    twice = 2.0 / sigma
    factors_ref[0] = sigma / half
    factors_ref[1] = jnp.zeros_like(sigma)
    for degree in range(1, DEGREE):
        following = 1.0 / (twice - sigma)
        factors_ref[2 * degree] = 2.0 * following / half
        factors_ref[2 * degree + 1] = sigma * following
        sigma = following
    middle = middle[:1]
    table = table_ref[...]
    slot = jnp.right_shift(table - (rows + 1), 6)
    offset = slot - jnp.where(slot < REACH, REACH, REACH - 1)
    source = jnp.bitwise_and(place - offset, GROUP - 1)
    halo = source * 64 + jnp.bitwise_and(table - (rows + 1), 63)
    halo_table[...] = jnp.where(table > rows, halo, -1)

    def gathered(names_ref, column, row):
        here = lax.broadcasted_iota(jnp.int32, (TILE, TILE), 0) + column
        total = jnp.zeros((TILE, TILE), F32)
        for neighbour in range(stencil):
            weight = -KINETIC_SCALE * DIFFERENCE_WEIGHTS[neighbour % SPAN + 1]
            names = names_ref[neighbour : neighbour + 1, row : row + TILE]
            total = total + jnp.where(here == names, weight, 0.0)
        return total, here

    for row in range(0, rows, TILE):
        diagonal = potential_ref[:, row : row + TILE] + (CENTRE_WEIGHT - middle)

        @pl.loop(0, rows // TILE)
        def _(block, row=row, diagonal=diagonal):
            column = pl.multiple_of(block * TILE, TILE)
            total, here = gathered(table_ref, column, row)
            right = lax.broadcasted_iota(jnp.int32, (TILE, TILE), 1) + row
            total = total + jnp.where(here == right, diagonal, 0.0)
            high, low = split(jnp.transpose(total))
            high_ref[pl.ds(row, TILE), pl.ds(column, TILE)] = high
            low_ref[pl.ds(row, TILE), pl.ds(column, TILE)] = low

    @pl.loop(0, GROUP * 64 // TILE)
    def _(block):
        column = pl.multiple_of(block * TILE, TILE)
        total, _ = gathered(halo_table, column, rows - TILE)
        high, low = split(jnp.transpose(total))
        halos_ref[pl.ds(0, TILE), pl.ds(column, TILE)] = high
        halos_ref[pl.ds(TILE, TILE), pl.ds(column, TILE)] = low

    local_part(start_ref[...], high_ref, low_ref, own_ref, part_ref, outgoing_ref)


def local_kernel(fields_ref, high_ref, low_ref, own_ref, part_ref, outgoing_ref):
    local_part(fields_ref[...], high_ref, low_ref, own_ref, part_ref, outgoing_ref)


def update_kernel(degree, factors_ref, part_ref, halo_ref, halos_ref, *rest):
    refs = list(rest)
    before_ref = refs.pop(0) if degree > 0 else None
    cross_ref = refs.pop(0) if degree < DEGREE - 1 else None
    fields_ref, extra_ref = refs
    scale = factors_ref[2 * degree][:1]
    carried = factors_ref[2 * degree + 1][:1]
    rows = part_ref.shape[0]
    reached = dot(halos_ref[...], halo_ref[...])
    reached = reached[:TILE] + reached[TILE:]
    for at in range(0, rows, TILE):
        image = part_ref[pl.ds(at, TILE), :]
        if at == rows - TILE:
            image = image + reached
        image = image * scale
        if degree > 0:
            image = image - carried * before_ref[pl.ds(at, TILE), :]
        fields_ref[pl.ds(at, TILE), :] = image
        if degree == DEGREE - 1:
            for copy in range(extra_ref.shape[0]):
                extra_ref[copy, pl.ds(at, TILE), :] = image.astype(BF16)
    if degree < DEGREE - 1:
        extra_ref[...] = dot(cross_ref[...], fields_ref[...].astype(BF16)).astype(BF16)


def end_kernel(scaling, fields_ref, summed_ref, filtered_ref, margin_ref):
    filtered_ref[...] = fields_ref[...]
    margin_ref[...] = summed_ref[...] * scaling


def margin_kernel(band_ref, every_ref, partial_ref):
    bands, _, width = every_ref.shape
    wanted = 2 * bands
    order = [band % 2 * (bands // 2) + band // 2 for band in range(bands)]
    row = lax.broadcasted_iota(jnp.int32, (wanted, width), 0)
    column = lax.broadcasted_iota(jnp.int32, (wanted, width), 1)
    target = jnp.right_shift(row, 1) * wanted + 2 * band_ref[0] + jnp.bitwise_and(row, 1)
    pick = jnp.where(column == target, 1.0, 0.0).astype(BF16)
    chosen = [
        lax.dot_general(pick, every_ref[order[band]], (((1,), (1,)), ((), ())), preferred_element_type=F32).astype(BF16)
        for band in range(bands)
    ]
    chosen = jnp.concatenate(chosen, axis=0)
    for band in range(bands):
        partial_ref[:, pl.ds(band * width, width)] = dot(chosen, every_ref[order[band]]).astype(BF16)


def call(kernel, operands, specs, outs, flops, scratch=()):
    moved = sum(x.size * x.dtype.itemsize for x in (*operands, *outs))
    return pl.pallas_call(
        kernel,
        out_shape=tuple(outs),
        in_specs=specs,
        out_specs=tuple(VMEM for _ in outs),
        scratch_shapes=list(scratch),
        compiler_params=pltpu.CompilerParams(vmem_limit_bytes=16 * 1024 * 1024),
        cost_estimate=pl.CostEstimate(flops=flops, bytes_accessed=moved, transcendentals=0),
    )(*operands)


def shape(dims, dtype=F32):
    return jax.ShapeDtypeStruct(dims, dtype)


def across(crossing, parts):
    route = []
    for at in range(parts):
        place = at % GROUP
        if place >= 5 and at + GROUP < parts:
            route.append((at, at + GROUP))
        if place <= 2 and at >= GROUP:
            route.append((at, at - GROUP))
    return lax.ppermute(crossing, "grid", route)


def exchanged(outgoing, relayed, place, parts):
    zeros = jnp.zeros_like(relayed)
    down = jnp.where(place >= 5, relayed, zeros)
    up = jnp.where(place <= 2, relayed, zeros)
    gap = jnp.zeros((outgoing.shape[0] - 2 * relayed.shape[0], relayed.shape[1]), BF16)
    message = (outgoing + jnp.concatenate([down, gap, up], axis=0)).reshape(GROUP, -1, outgoing.shape[1])
    groups = [list(range(first, first + GROUP)) for first in range(0, parts, GROUP)]
    received = lax.all_to_all(message, "grid", 0, 0, axis_index_groups=groups, tiled=True)
    return received.reshape(outgoing.shape)


def on_device(states, potential, bounds, point_count, send_rows, stencil_table):
    rows, width = states.shape
    stencil = stencil_table.shape[0]
    parts = lax.axis_size("grid")
    bands = lax.axis_size("band")
    slots = GROUP * 64
    place = jnp.bitwise_and(lax.axis_index("grid"), GROUP - 1).reshape(1)
    band = lax.axis_index("band").reshape(1)

    start, own, cross, crossing = call(
        begin_kernel,
        (place, band, point_count, jnp.swapaxes(send_rows, 0, 1), states),
        [SMEM, SMEM, SMEM, VMEM, VMEM],
        [shape((rows, width)), shape((slots, rows), BF16), shape((REACH * 64, rows), BF16), shape((REACH * 64, width), BF16)],
        10_000_000,
    )
    relayed = across(crossing, parts)
    high, low, halos, factors, part, outgoing = call(
        build_kernel,
        (place, bounds.reshape(1, 3), potential.reshape(1, rows), stencil_table, start, own),
        [SMEM, VMEM, VMEM, VMEM, VMEM, VMEM],
        [
            shape((rows, rows), BF16),
            shape((rows, rows), BF16),
            shape((2 * TILE, slots), BF16),
            shape((2 * DEGREE, 8, TILE)),
            shape((rows, width)),
            shape((slots, width), BF16),
        ],
        50_000_000,
        [pltpu.VMEM((stencil, rows), jnp.int32)],
    )
    before, fields = None, start
    for degree in range(DEGREE):
        if degree > 0:
            relayed = across(extra, parts)
            part, outgoing = call(
                local_kernel,
                (fields, high, low, own),
                [VMEM] * 4,
                [shape((rows, width)), shape((slots, width), BF16)],
                80_000_000,
            )
        halo = exchanged(outgoing, relayed, place[0], parts)
        operands = [factors, part, halo, halos]
        if degree > 0:
            operands.append(before)
        if degree < DEGREE - 1:
            operands.append(cross)
            after = shape((REACH * 64, width), BF16)
        else:
            after = shape((bands // 2, rows, width), BF16)
        before = fields
        fields, extra = call(
            functools.partial(update_kernel, degree),
            operands,
            [VMEM] * len(operands),
            [shape((rows, width)), after],
            40_000_000,
        )
    alike = [list(range(core, bands, 2)) for core in range(2)]
    chips = [[first, first + 1] for first in range(0, bands, 2)]
    alike_bands = lax.all_to_all(extra, "band", 0, 0, axis_index_groups=alike, tiled=True)
    every_band = lax.all_gather(alike_bands, "band", axis=0, axis_index_groups=chips, tiled=True)
    (partial_sums,) = call(
        margin_kernel,
        (band, every_band),
        [SMEM, VMEM],
        [shape((2 * parts, bands * width), BF16)],
        80_000_000,
    )
    blocks = lax.all_to_all(partial_sums.reshape(parts, 2, bands * width), "grid", 0, 0, tiled=True)
    summed = jnp.sum(blocks.astype(F32), axis=0)
    return call(
        functools.partial(end_kernel, 1.0 / (parts * rows)),
        (fields, summed),
        [VMEM, VMEM],
        [shape((rows, width)), shape(summed.shape)],
        1000,
    )


def solution(mesh):
    placed = (P("grid", "band"), P("grid"), P(), P("grid"), P("grid", None, None), P(None, "grid"))
    return jax.shard_map(
        on_device,
        mesh=mesh,
        in_specs=placed,
        out_specs=(P("grid", "band"), P(("grid", "band"), None)),
        check_vma=False,
    )
```

```python
import functools

import jax
import jax.numpy as jnp
from jax import lax
from jax.experimental import pallas as pl
from jax.experimental.pallas import tpu as pltpu
from jax.sharding import PartitionSpec as P

SPAN = 6
DEGREE = 3
REACH = 3
GROUP = 8

DIFFERENCE_WEIGHTS = (
    -5369.0 / 1800.0,
    12.0 / 7.0,
    -15.0 / 56.0,
    10.0 / 189.0,
    -1.0 / 112.0,
    2.0 / 1925.0,
    -1.0 / 16632.0,
)
KINETIC_SCALE = 0.5 / 0.49
CENTRE_WEIGHT = -3.0 * KINETIC_SCALE * DIFFERENCE_WEIGHTS[0]
TILE = 128
BF16 = jnp.bfloat16
F32 = jnp.float32
VMEM = pl.BlockSpec(memory_space=pltpu.VMEM)
SMEM = pl.BlockSpec(memory_space=pltpu.SMEM)


def dot(a, b):
    return jnp.dot(a, b, preferred_element_type=F32)


def split(values):
    high = values.astype(BF16)
    return high, (values - high.astype(F32)).astype(BF16)


def select_rows(select_ref, sends_ref, offsets, rows):
    def block(offset):
        picks = jnp.full((1, 64), rows, jnp.int32)
        for slot in range(2 * REACH):
            kept = slot - REACH if slot < REACH else slot - REACH + 1
            picks = jnp.where(offset == kept, sends_ref[slot], picks)
        return picks

    for pair in range((len(offsets) + 1) // 2):
        two = [block(offset) for offset in offsets[2 * pair : 2 * pair + 2]]
        height = 64 * len(two)
        picks = jnp.concatenate([two[0], two[-1]], axis=1)
        for at in range(0, rows, TILE):
            here = lax.broadcasted_iota(jnp.int32, (TILE, TILE), 0) + at
            hit = jnp.where(here == picks, 1.0, 0.0)
            select_ref[pl.ds(pair * TILE, height), pl.ds(at, TILE)] = jnp.transpose(hit)[:height].astype(BF16)


def begin_kernel(
    place_ref, band_ref, sends_ref, states_ref, held_ref, own_ref, cross_ref, crossing_ref
):
    place = place_ref[0]
    rows = states_ref.shape[0]
    first = jnp.where(place >= 5, GROUP - place, -REACH - place)
    select_rows(cross_ref, sends_ref, [first + at for at in range(REACH)], rows)
    crossing_ref[...] = dot(cross_ref[...], states_ref[...].astype(BF16)).astype(BF16)
    held_ref[...] = states_ref[...]
    select_rows(own_ref, sends_ref, [at - place for at in range(GROUP)], rows)


def local_part(fields, high_ref, low_ref, own_ref, part_ref, outgoing_ref):
    high, low = split(fields)
    part_ref[...] = dot(high_ref[...], high) + dot(low_ref[...], high) + dot(high_ref[...], low)
    outgoing_ref[...] = dot(own_ref[...], high).astype(BF16)


def build_kernel(
    place_ref, count_ref, bounds_ref, potential_ref, table_ref, states_ref, own_ref, start_ref,
    high_ref, low_ref, halos_ref, factors_ref, part_ref, outgoing_ref, halo_table
):
    place = place_ref[0]
    rows = states_ref.shape[0]
    stencil = table_ref.shape[0]
    lower, cutoff, upper = (jnp.broadcast_to(bounds_ref[:, at : at + 1], (8, TILE)) for at in range(3))
    half = (upper - cutoff) / 2.0
    middle = (upper + cutoff) / 2.0
    sigma = half / (lower - middle)
    twice = 2.0 / sigma
    factors_ref[0] = sigma / half
    factors_ref[1] = jnp.zeros_like(sigma)
    for degree in range(1, DEGREE):
        following = 1.0 / (twice - sigma)
        factors_ref[2 * degree] = 2.0 * following / half
        factors_ref[2 * degree + 1] = sigma * following
        sigma = following
    middle = middle[:1]
    table = table_ref[...]
    slot = jnp.right_shift(table - (rows + 1), 6)
    offset = slot - jnp.where(slot < REACH, REACH, REACH - 1)
    source = jnp.bitwise_and(place - offset, GROUP - 1)
    halo = source * 64 + jnp.bitwise_and(table - (rows + 1), 63)
    halo_table[...] = jnp.where(table > rows, halo, -1)

    def gathered(names_ref, column, row):
        here = lax.broadcasted_iota(jnp.int32, (TILE, TILE), 0) + column
        total = jnp.zeros((TILE, TILE), F32)
        for neighbour in range(stencil):
            weight = -KINETIC_SCALE * DIFFERENCE_WEIGHTS[neighbour % SPAN + 1]
            names = names_ref[neighbour : neighbour + 1, row : row + TILE]
            total = total + jnp.where(here == names, weight, 0.0)
        return total, here

    for row in range(0, rows, TILE):
        diagonal = potential_ref[:, row : row + TILE] + (CENTRE_WEIGHT - middle)

        @pl.loop(0, rows // TILE)
        def _(block, row=row, diagonal=diagonal):
            column = pl.multiple_of(block * TILE, TILE)
            total, here = gathered(table_ref, column, row)
            right = lax.broadcasted_iota(jnp.int32, (TILE, TILE), 1) + row
            total = total + jnp.where(here == right, diagonal, 0.0)
            high, low = split(jnp.transpose(total))
            high_ref[pl.ds(row, TILE), pl.ds(column, TILE)] = high
            low_ref[pl.ds(row, TILE), pl.ds(column, TILE)] = low

    @pl.loop(0, GROUP * 64 // TILE)
    def _(block):
        column = pl.multiple_of(block * TILE, TILE)
        total, _ = gathered(halo_table, column, rows - TILE)
        high, low = split(jnp.transpose(total))
        halos_ref[pl.ds(0, TILE), pl.ds(column, TILE)] = high
        halos_ref[pl.ds(TILE, TILE), pl.ds(column, TILE)] = low

    live = lax.broadcasted_iota(jnp.int32, states_ref.shape, 0) < count_ref[0]
    start_ref[...] = jnp.where(live, states_ref[...], 0.0)
    local_part(start_ref[...], high_ref, low_ref, own_ref, part_ref, outgoing_ref)


def local_kernel(fields_ref, high_ref, low_ref, own_ref, part_ref, outgoing_ref):
    local_part(fields_ref[...], high_ref, low_ref, own_ref, part_ref, outgoing_ref)


def update_kernel(degree, factors_ref, part_ref, halo_ref, halos_ref, *rest):
    refs = list(rest)
    before_ref = refs.pop(0) if degree > 0 else None
    cross_ref = refs.pop(0) if degree < DEGREE - 1 else None
    fields_ref, extra_ref = refs
    scale = factors_ref[2 * degree][:1]
    carried = factors_ref[2 * degree + 1][:1]
    rows = part_ref.shape[0]
    reached = dot(halos_ref[...], halo_ref[...])
    reached = reached[:TILE] + reached[TILE:]
    for at in range(0, rows, TILE):
        image = part_ref[pl.ds(at, TILE), :]
        if at == rows - TILE:
            image = image + reached
        image = image * scale
        if degree > 0:
            image = image - carried * before_ref[pl.ds(at, TILE), :]
        fields_ref[pl.ds(at, TILE), :] = image
        if degree == DEGREE - 1:
            for copy in range(extra_ref.shape[0]):
                extra_ref[copy, pl.ds(at, TILE), :] = image.astype(BF16)
    if degree < DEGREE - 1:
        extra_ref[...] = dot(cross_ref[...], fields_ref[...].astype(BF16)).astype(BF16)


def end_kernel(scaling, fields_ref, summed_ref, filtered_ref, margin_ref):
    filtered_ref[...] = fields_ref[...]
    margin_ref[...] = summed_ref[...] * scaling


def margin_kernel(band_ref, every_ref, partial_ref):
    bands, _, width = every_ref.shape
    wanted = 2 * bands
    order = [band % 2 * (bands // 2) + band // 2 for band in range(bands)]
    row = lax.broadcasted_iota(jnp.int32, (wanted, width), 0)
    column = lax.broadcasted_iota(jnp.int32, (wanted, width), 1)
    target = jnp.right_shift(row, 1) * wanted + 2 * band_ref[0] + jnp.bitwise_and(row, 1)
    pick = jnp.where(column == target, 1.0, 0.0).astype(BF16)
    chosen = [
        lax.dot_general(pick, every_ref[order[band]], (((1,), (1,)), ((), ())), preferred_element_type=F32).astype(BF16)
        for band in range(bands)
    ]
    chosen = jnp.concatenate(chosen, axis=0)
    for band in range(bands):
        partial_ref[:, pl.ds(band * width, width)] = dot(chosen, every_ref[order[band]]).astype(BF16)


def call(kernel, operands, specs, outs, flops, scratch=()):
    moved = sum(x.size * x.dtype.itemsize for x in (*operands, *outs))
    return pl.pallas_call(
        kernel,
        out_shape=tuple(outs),
        in_specs=specs,
        out_specs=tuple(VMEM for _ in outs),
        scratch_shapes=list(scratch),
        compiler_params=pltpu.CompilerParams(vmem_limit_bytes=16 * 1024 * 1024),
        cost_estimate=pl.CostEstimate(flops=flops, bytes_accessed=moved, transcendentals=0),
    )(*operands)


def shape(dims, dtype=F32):
    return jax.ShapeDtypeStruct(dims, dtype)


def across(crossing, parts):
    route = []
    for at in range(parts):
        place = at % GROUP
        if place >= 5 and at + GROUP < parts:
            route.append((at, at + GROUP))
        if place <= 2 and at >= GROUP:
            route.append((at, at - GROUP))
    return lax.ppermute(crossing, "grid", route)


def exchanged(outgoing, relayed, place, parts):
    zeros = jnp.zeros_like(relayed)
    down = jnp.where(place >= 5, relayed, zeros)
    up = jnp.where(place <= 2, relayed, zeros)
    gap = jnp.zeros((outgoing.shape[0] - 2 * relayed.shape[0], relayed.shape[1]), BF16)
    message = (outgoing + jnp.concatenate([down, gap, up], axis=0)).reshape(GROUP, -1, outgoing.shape[1])
    groups = [list(range(first, first + GROUP)) for first in range(0, parts, GROUP)]
    received = lax.all_to_all(message, "grid", 0, 0, axis_index_groups=groups, tiled=True)
    return received.reshape(outgoing.shape)


def on_device(states, potential, bounds, point_count, send_rows, stencil_table):
    rows, width = states.shape
    stencil = stencil_table.shape[0]
    parts = lax.axis_size("grid")
    bands = lax.axis_size("band")
    slots = GROUP * 64
    place = jnp.bitwise_and(lax.axis_index("grid"), GROUP - 1).reshape(1)
    band = lax.axis_index("band").reshape(1)

    held, own, cross, crossing = call(
        begin_kernel,
        (place, band, jnp.swapaxes(send_rows, 0, 1), states),
        [SMEM, SMEM, VMEM, VMEM],
        [shape((rows, width)), shape((slots, rows), BF16), shape((REACH * 64, rows), BF16), shape((REACH * 64, width), BF16)],
        10_000_000,
    )
    relayed = across(crossing, parts)
    start, high, low, halos, factors, part, outgoing = call(
        build_kernel,
        (place, point_count, bounds.reshape(1, 3), potential.reshape(1, rows), stencil_table, held, own),
        [SMEM, SMEM, VMEM, VMEM, VMEM, VMEM, VMEM],
        [
            shape((rows, width)),
            shape((rows, rows), BF16),
            shape((rows, rows), BF16),
            shape((2 * TILE, slots), BF16),
            shape((2 * DEGREE, 8, TILE)),
            shape((rows, width)),
            shape((slots, width), BF16),
        ],
        50_000_000,
        [pltpu.VMEM((stencil, rows), jnp.int32)],
    )
    before, fields = None, start
    for degree in range(DEGREE):
        if degree > 0:
            relayed = across(extra, parts)
            part, outgoing = call(
                local_kernel,
                (fields, high, low, own),
                [VMEM] * 4,
                [shape((rows, width)), shape((slots, width), BF16)],
                80_000_000,
            )
        halo = exchanged(outgoing, relayed, place[0], parts)
        operands = [factors, part, halo, halos]
        if degree > 0:
            operands.append(before)
        if degree < DEGREE - 1:
            operands.append(cross)
            after = shape((REACH * 64, width), BF16)
        else:
            after = shape((bands // 2, rows, width), BF16)
        before = fields
        fields, extra = call(
            functools.partial(update_kernel, degree),
            operands,
            [VMEM] * len(operands),
            [shape((rows, width)), after],
            40_000_000,
        )
    alike = [list(range(core, bands, 2)) for core in range(2)]
    chips = [[first, first + 1] for first in range(0, bands, 2)]
    alike_bands = lax.all_to_all(extra, "band", 0, 0, axis_index_groups=alike, tiled=True)
    every_band = lax.all_gather(alike_bands, "band", axis=0, axis_index_groups=chips, tiled=True)
    (partial_sums,) = call(
        margin_kernel,
        (band, every_band),
        [SMEM, VMEM],
        [shape((2 * parts, bands * width), BF16)],
        80_000_000,
    )
    blocks = lax.all_to_all(partial_sums.reshape(parts, 2, bands * width), "grid", 0, 0, tiled=True)
    summed = jnp.sum(blocks.astype(F32), axis=0)
    return call(
        functools.partial(end_kernel, 1.0 / (parts * rows)),
        (fields, summed),
        [VMEM, VMEM],
        [shape((rows, width)), shape(summed.shape)],
        1000,
    )


def solution(mesh):
    placed = (P("grid", "band"), P("grid"), P(), P("grid"), P("grid", None, None), P(None, "grid"))
    return jax.shard_map(
        on_device,
        mesh=mesh,
        in_specs=placed,
        out_specs=(P("grid", "band"), P(("grid", "band"), None)),
        check_vma=False,
    )
```

```python
import functools

import jax
import jax.numpy as jnp
from jax import lax
from jax.experimental import pallas as pl
from jax.experimental.pallas import tpu as pltpu
from jax.sharding import PartitionSpec as P

SPAN = 6
DEGREE = 3
REACH = 3
GROUP = 8

DIFFERENCE_WEIGHTS = (
    -5369.0 / 1800.0,
    12.0 / 7.0,
    -15.0 / 56.0,
    10.0 / 189.0,
    -1.0 / 112.0,
    2.0 / 1925.0,
    -1.0 / 16632.0,
)
KINETIC_SCALE = 0.5 / 0.49
CENTRE_WEIGHT = -3.0 * KINETIC_SCALE * DIFFERENCE_WEIGHTS[0]
TILE = 128
BF16 = jnp.bfloat16
F32 = jnp.float32
VMEM = pl.BlockSpec(memory_space=pltpu.VMEM)
SMEM = pl.BlockSpec(memory_space=pltpu.SMEM)


def dot(a, b):
    return jnp.dot(a, b, preferred_element_type=F32)


def split(values):
    high = values.astype(BF16)
    return high, (values - high.astype(F32)).astype(BF16)


def select_rows(select_ref, sends_ref, offsets, rows):
    def block(offset):
        picks = jnp.full((1, 64), rows, jnp.int32)
        for slot in range(2 * REACH):
            kept = slot - REACH if slot < REACH else slot - REACH + 1
            picks = jnp.where(offset == kept, sends_ref[slot], picks)
        return picks

    for pair in range((len(offsets) + 1) // 2):
        two = [block(offset) for offset in offsets[2 * pair : 2 * pair + 2]]
        height = 64 * len(two)
        picks = jnp.concatenate([two[0], two[-1]], axis=1)
        for at in range(0, rows, TILE):
            here = lax.broadcasted_iota(jnp.int32, (TILE, TILE), 0) + at
            hit = jnp.where(here == picks, 1.0, 0.0)
            select_ref[pl.ds(pair * TILE, height), pl.ds(at, TILE)] = jnp.transpose(hit)[:height].astype(BF16)


def begin_kernel(
    place_ref, band_ref, sends_ref, states_ref, held_ref, own_ref, cross_ref, crossing_ref
):
    place = place_ref[0]
    rows = states_ref.shape[0]
    first = jnp.where(place >= 5, GROUP - place, -REACH - place)
    select_rows(cross_ref, sends_ref, [first + at for at in range(REACH)], rows)
    crossing_ref[...] = dot(cross_ref[...], states_ref[...].astype(BF16)).astype(BF16)
    held_ref[...] = states_ref[...]
    select_rows(own_ref, sends_ref, [at - place for at in range(GROUP)], rows)


def local_part(fields, high_ref, low_ref, own_ref, part_ref, outgoing_ref):
    high, low = split(fields)
    part_ref[...] = dot(high_ref[...], high) + dot(low_ref[...], high) + dot(high_ref[...], low)
    outgoing_ref[...] = dot(own_ref[...], high).astype(BF16)


def build_kernel(
    bounds_ref, potential_ref, table_ref, states_ref, own_ref,
    high_ref, low_ref, halos_ref, factors_ref, part_ref, outgoing_ref
):
    rows = states_ref.shape[0]
    stencil = table_ref.shape[0]
    lower, cutoff, upper = (jnp.broadcast_to(bounds_ref[:, at : at + 1], (8, TILE)) for at in range(3))
    half = (upper - cutoff) / 2.0
    middle = (upper + cutoff) / 2.0
    sigma = half / (lower - middle)
    twice = 2.0 / sigma
    factors_ref[0] = sigma / half
    factors_ref[1] = jnp.zeros_like(sigma)
    for degree in range(1, DEGREE):
        following = 1.0 / (twice - sigma)
        factors_ref[2 * degree] = 2.0 * following / half
        factors_ref[2 * degree + 1] = sigma * following
        sigma = following
    middle = middle[:1]
    def gathered(column, row):
        here = lax.broadcasted_iota(jnp.int32, (TILE, TILE), 0) + column
        total = jnp.zeros((TILE, TILE), F32)
        for neighbour in range(stencil):
            weight = -KINETIC_SCALE * DIFFERENCE_WEIGHTS[neighbour % SPAN + 1]
            names = table_ref[neighbour : neighbour + 1, row : row + TILE]
            total = total + jnp.where(here == names, weight, 0.0)
        return total, here

    for row in range(0, rows, TILE):
        diagonal = potential_ref[:, row : row + TILE] + (CENTRE_WEIGHT - middle)

        @pl.loop(0, rows // TILE)
        def _(block, row=row, diagonal=diagonal):
            column = pl.multiple_of(block * TILE, TILE)
            total, here = gathered(column, row)
            right = lax.broadcasted_iota(jnp.int32, (TILE, TILE), 1) + row
            total = total + jnp.where(here == right, diagonal, 0.0)
            high, low = split(jnp.transpose(total))
            high_ref[pl.ds(row, TILE), pl.ds(column, TILE)] = high
            low_ref[pl.ds(row, TILE), pl.ds(column, TILE)] = low

    @pl.loop(0, 2 * REACH * 64 // TILE)
    def _(block):
        column = pl.multiple_of(block * TILE, TILE)
        total, _ = gathered(column + rows + 1, rows - TILE)
        high, low = split(jnp.transpose(total))
        halos_ref[pl.ds(0, TILE), pl.ds(column, TILE)] = high
        halos_ref[pl.ds(TILE, TILE), pl.ds(column, TILE)] = low

    local_part(states_ref[...], high_ref, low_ref, own_ref, part_ref, outgoing_ref)


def masking_kernel(
    count_ref, states_ref, fields_ref, high_ref, low_ref, own_ref, start_ref, masked_ref, part_ref, outgoing_ref
):
    live = lax.broadcasted_iota(jnp.int32, states_ref.shape, 0) < count_ref[0]
    start_ref[...] = jnp.where(live, states_ref[...], 0.0)
    masked_ref[...] = jnp.where(live, fields_ref[...], 0.0)
    local_part(masked_ref[...], high_ref, low_ref, own_ref, part_ref, outgoing_ref)


def local_kernel(fields_ref, high_ref, low_ref, own_ref, part_ref, outgoing_ref):
    local_part(fields_ref[...], high_ref, low_ref, own_ref, part_ref, outgoing_ref)


def update_kernel(degree, place_ref, factors_ref, part_ref, halo_ref, halos_ref, *rest):
    refs = list(rest)
    before_ref = refs.pop(0) if degree > 0 else None
    cross_ref = refs.pop(0) if degree < DEGREE - 1 else None
    fields_ref, extra_ref = refs
    scale = factors_ref[2 * degree][:1]
    carried = factors_ref[2 * degree + 1][:1]
    rows = part_ref.shape[0]
    blocks = []
    for slot in range(2 * REACH):
        offset = slot - REACH if slot < REACH else slot - REACH + 1
        blocks.append(halo_ref[jnp.bitwise_and(place_ref[0] - offset, GROUP - 1)])
    reached = dot(halos_ref[...], jnp.concatenate(blocks, axis=0))
    reached = reached[:TILE] + reached[TILE:]
    for at in range(0, rows, TILE):
        image = part_ref[pl.ds(at, TILE), :]
        if at == rows - TILE:
            image = image + reached
        image = image * scale
        if degree > 0:
            image = image - carried * before_ref[pl.ds(at, TILE), :]
        fields_ref[pl.ds(at, TILE), :] = image
        if degree == DEGREE - 1:
            for copy in range(extra_ref.shape[0]):
                extra_ref[copy, pl.ds(at, TILE), :] = image.astype(BF16)
    if degree < DEGREE - 1:
        extra_ref[...] = dot(cross_ref[...], fields_ref[...].astype(BF16)).astype(BF16)


def end_kernel(scaling, fields_ref, summed_ref, filtered_ref, margin_ref):
    filtered_ref[...] = fields_ref[...]
    margin_ref[...] = summed_ref[...] * scaling


def margin_kernel(band_ref, every_ref, partial_ref):
    bands, _, width = every_ref.shape
    wanted = 2 * bands
    order = [band % 2 * (bands // 2) + band // 2 for band in range(bands)]
    row = lax.broadcasted_iota(jnp.int32, (wanted, width), 0)
    column = lax.broadcasted_iota(jnp.int32, (wanted, width), 1)
    target = jnp.right_shift(row, 1) * wanted + 2 * band_ref[0] + jnp.bitwise_and(row, 1)
    pick = jnp.where(column == target, 1.0, 0.0).astype(BF16)
    chosen = [
        lax.dot_general(pick, every_ref[order[band]], (((1,), (1,)), ((), ())), preferred_element_type=F32).astype(BF16)
        for band in range(bands)
    ]
    chosen = jnp.concatenate(chosen, axis=0)
    for band in range(bands):
        partial_ref[:, pl.ds(band * width, width)] = dot(chosen, every_ref[order[band]]).astype(BF16)


def call(kernel, operands, specs, outs, flops, scratch=()):
    moved = sum(x.size * x.dtype.itemsize for x in (*operands, *outs))
    return pl.pallas_call(
        kernel,
        out_shape=tuple(outs),
        in_specs=specs,
        out_specs=tuple(VMEM for _ in outs),
        scratch_shapes=list(scratch),
        compiler_params=pltpu.CompilerParams(vmem_limit_bytes=16 * 1024 * 1024),
        cost_estimate=pl.CostEstimate(flops=flops, bytes_accessed=moved, transcendentals=0),
    )(*operands)


def shape(dims, dtype=F32):
    return jax.ShapeDtypeStruct(dims, dtype)


def across(crossing, parts):
    route = []
    for at in range(parts):
        place = at % GROUP
        if place >= 5 and at + GROUP < parts:
            route.append((at, at + GROUP))
        if place <= 2 and at >= GROUP:
            route.append((at, at - GROUP))
    return lax.ppermute(crossing, "grid", route)


def exchanged(outgoing, relayed, place, parts):
    zeros = jnp.zeros_like(relayed)
    down = jnp.where(place >= 5, relayed, zeros)
    up = jnp.where(place <= 2, relayed, zeros)
    gap = jnp.zeros((outgoing.shape[0] - 2 * relayed.shape[0], relayed.shape[1]), BF16)
    message = (outgoing + jnp.concatenate([down, gap, up], axis=0)).reshape(GROUP, -1, outgoing.shape[1])
    groups = [list(range(first, first + GROUP)) for first in range(0, parts, GROUP)]
    received = lax.all_to_all(message, "grid", 0, 0, axis_index_groups=groups, tiled=True)
    return received


def on_device(states, potential, bounds, point_count, send_rows, stencil_table):
    rows, width = states.shape
    parts = lax.axis_size("grid")
    bands = lax.axis_size("band")
    slots = GROUP * 64
    place = jnp.bitwise_and(lax.axis_index("grid"), GROUP - 1).reshape(1)
    band = lax.axis_index("band").reshape(1)

    held, own, cross, crossing = call(
        begin_kernel,
        (place, band, jnp.swapaxes(send_rows, 0, 1), states),
        [SMEM, SMEM, VMEM, VMEM],
        [shape((rows, width)), shape((slots, rows), BF16), shape((REACH * 64, rows), BF16), shape((REACH * 64, width), BF16)],
        10_000_000,
    )
    relayed = across(crossing, parts)
    high, low, halos, factors, part, outgoing = call(
        build_kernel,
        (bounds.reshape(1, 3), potential.reshape(1, rows), stencil_table, held, own),
        [VMEM] * 5,
        [
            shape((rows, rows), BF16),
            shape((rows, rows), BF16),
            shape((2 * TILE, 2 * REACH * 64), BF16),
            shape((2 * DEGREE, 8, TILE)),
            shape((rows, width)),
            shape((slots, width), BF16),
        ],
        50_000_000,
    )
    before, fields = None, held
    for degree in range(DEGREE):
        if degree > 0:
            relayed = across(extra, parts)
            operands = [fields, high, low, own]
            outs = [shape((rows, width)), shape((slots, width), BF16)]
            if degree == 1:
                before, fields, part, outgoing = call(
                    masking_kernel,
                    [point_count, before] + operands,
                    [SMEM] + [VMEM] * 5,
                    [shape((rows, width))] * 2 + outs,
                    80_000_000,
                )
            else:
                part, outgoing = call(local_kernel, operands, [VMEM] * 4, outs, 80_000_000)
        halo = exchanged(outgoing, relayed, place[0], parts)
        operands = [place, factors, part, halo, halos]
        if degree > 0:
            operands.append(before)
        if degree < DEGREE - 1:
            operands.append(cross)
            after = shape((REACH * 64, width), BF16)
        else:
            after = shape((bands // 2, rows, width), BF16)
        before = fields
        fields, extra = call(
            functools.partial(update_kernel, degree),
            operands,
            [SMEM] + [VMEM] * (len(operands) - 1),
            [shape((rows, width)), after],
            40_000_000,
        )
    alike = [list(range(core, bands, 2)) for core in range(2)]
    chips = [[first, first + 1] for first in range(0, bands, 2)]
    alike_bands = lax.all_to_all(extra, "band", 0, 0, axis_index_groups=alike, tiled=True)
    every_band = lax.all_gather(alike_bands, "band", axis=0, axis_index_groups=chips, tiled=True)
    (partial_sums,) = call(
        margin_kernel,
        (band, every_band),
        [SMEM, VMEM],
        [shape((2 * parts, bands * width), BF16)],
        80_000_000,
    )
    blocks = lax.all_to_all(partial_sums.reshape(parts, 2, bands * width), "grid", 0, 0, tiled=True)
    summed = jnp.sum(blocks.astype(F32), axis=0)
    return call(
        functools.partial(end_kernel, 1.0 / (parts * rows)),
        (fields, summed),
        [VMEM, VMEM],
        [shape((rows, width)), shape(summed.shape)],
        1000,
    )


def solution(mesh):
    placed = (P("grid", "band"), P("grid"), P(), P("grid"), P("grid", None, None), P(None, "grid"))
    return jax.shard_map(
        on_device,
        mesh=mesh,
        in_specs=placed,
        out_specs=(P("grid", "band"), P(("grid", "band"), None)),
        check_vma=False,
    )
```

```python
import functools

import jax
import jax.numpy as jnp
from jax import lax
from jax.experimental import pallas as pl
from jax.experimental.pallas import tpu as pltpu
from jax.sharding import PartitionSpec as P

SPAN = 6
DEGREE = 3
REACH = 3
GROUP = 8

DIFFERENCE_WEIGHTS = (
    -5369.0 / 1800.0,
    12.0 / 7.0,
    -15.0 / 56.0,
    10.0 / 189.0,
    -1.0 / 112.0,
    2.0 / 1925.0,
    -1.0 / 16632.0,
)
KINETIC_SCALE = 0.5 / 0.49
CENTRE_WEIGHT = -3.0 * KINETIC_SCALE * DIFFERENCE_WEIGHTS[0]
TILE = 128
BF16 = jnp.bfloat16
F32 = jnp.float32
VMEM = pl.BlockSpec(memory_space=pltpu.VMEM)
SMEM = pl.BlockSpec(memory_space=pltpu.SMEM)


def dot(a, b):
    return jnp.dot(a, b, preferred_element_type=F32)


def split(values):
    high = values.astype(BF16)
    return high, (values - high.astype(F32)).astype(BF16)


def select_rows(select_ref, sends_ref, offsets, rows):
    sends = sends_ref[...].astype(F32).astype(jnp.int32)

    def block(offset):
        picks = jnp.full((1, 64), rows, jnp.int32)
        for slot in range(2 * REACH):
            kept = slot - REACH if slot < REACH else slot - REACH + 1
            picks = jnp.where(offset == kept, sends[slot : slot + 1, :], picks)
        return picks

    for pair in range((len(offsets) + 1) // 2):
        two = [block(offset) for offset in offsets[2 * pair : 2 * pair + 2]]
        height = 64 * len(two)
        picks = jnp.concatenate([two[0], two[-1]], axis=1)
        for at in range(0, rows, TILE):
            here = lax.broadcasted_iota(jnp.int32, (TILE, TILE), 0) + at
            hit = jnp.where(here == picks, 1.0, 0.0)
            select_ref[pl.ds(pair * TILE, height), pl.ds(at, TILE)] = jnp.transpose(hit)[:height].astype(BF16)


def begin_kernel(
    place_ref, band_ref, sends_ref, states_ref, own_ref, cross_ref, crossing_ref
):
    place = place_ref[0]
    rows = states_ref.shape[0]
    first = jnp.where(place >= 5, GROUP - place, -REACH - place)
    select_rows(cross_ref, sends_ref, [first + at for at in range(REACH)], rows)
    crossing_ref[...] = dot(cross_ref[...], states_ref[...]).astype(BF16)
    select_rows(own_ref, sends_ref, [at - place for at in range(GROUP)], rows)


def local_part(fields, high_ref, low_ref, own_ref, part_ref, outgoing_ref):
    high, low = split(fields)
    part_ref[...] = dot(high_ref[...], high) + dot(low_ref[...], high) + dot(high_ref[...], low)
    outgoing_ref[...] = dot(own_ref[...], high).astype(BF16)


def build_kernel(
    bounds_ref, potential_ref, table_ref, states_ref, own_ref,
    high_ref, low_ref, halos_ref, factors_ref, part_ref, outgoing_ref
):
    rows = states_ref.shape[0]
    stencil = table_ref.shape[0]
    lower, cutoff, upper = (jnp.broadcast_to(bounds_ref[:, at : at + 1], (8, TILE)) for at in range(3))
    half = (upper - cutoff) / 2.0
    middle = (upper + cutoff) / 2.0
    sigma = half / (lower - middle)
    twice = 2.0 / sigma
    factors_ref[0] = sigma / half
    factors_ref[1] = jnp.zeros_like(sigma)
    for degree in range(1, DEGREE):
        following = 1.0 / (twice - sigma)
        factors_ref[2 * degree] = 2.0 * following / half
        factors_ref[2 * degree + 1] = sigma * following
        sigma = following
    middle = middle[:1]
    def gathered(column, row):
        here = lax.broadcasted_iota(jnp.int32, (TILE, TILE), 0) + column
        total = jnp.zeros((TILE, TILE), F32)
        for neighbour in range(stencil):
            weight = -KINETIC_SCALE * DIFFERENCE_WEIGHTS[neighbour % SPAN + 1]
            names = table_ref[neighbour : neighbour + 1, row : row + TILE]
            total = total + jnp.where(here == names, weight, 0.0)
        return total, here

    for row in range(0, rows, TILE):
        diagonal = potential_ref[:, row : row + TILE] + (CENTRE_WEIGHT - middle)

        @pl.loop(0, rows // TILE)
        def _(block, row=row, diagonal=diagonal):
            column = pl.multiple_of(block * TILE, TILE)
            total, here = gathered(column, row)
            right = lax.broadcasted_iota(jnp.int32, (TILE, TILE), 1) + row
            total = total + jnp.where(here == right, diagonal, 0.0)
            high, low = split(jnp.transpose(total))
            high_ref[pl.ds(row, TILE), pl.ds(column, TILE)] = high
            low_ref[pl.ds(row, TILE), pl.ds(column, TILE)] = low

    @pl.loop(0, 2 * REACH * 64 // TILE)
    def _(block):
        column = pl.multiple_of(block * TILE, TILE)
        total, _ = gathered(column + rows + 1, rows - TILE)
        high, low = split(jnp.transpose(total))
        halos_ref[pl.ds(0, TILE), pl.ds(column, TILE)] = high
        halos_ref[pl.ds(TILE, TILE), pl.ds(column, TILE)] = low

    local_part(states_ref[...], high_ref, low_ref, own_ref, part_ref, outgoing_ref)


def masking_kernel(
    count_ref, states_ref, fields_ref, high_ref, low_ref, own_ref, start_ref, masked_ref, part_ref, outgoing_ref
):
    live = lax.broadcasted_iota(jnp.int32, states_ref.shape, 0) < count_ref[0]
    start_ref[...] = jnp.where(live, states_ref[...], 0.0)
    masked_ref[...] = jnp.where(live, fields_ref[...], 0.0)
    local_part(masked_ref[...], high_ref, low_ref, own_ref, part_ref, outgoing_ref)


def local_kernel(fields_ref, high_ref, low_ref, own_ref, part_ref, outgoing_ref):
    local_part(fields_ref[...], high_ref, low_ref, own_ref, part_ref, outgoing_ref)


def update_kernel(degree, place_ref, factors_ref, part_ref, halo_ref, halos_ref, *rest):
    refs = list(rest)
    before_ref = refs.pop(0) if degree > 0 else None
    cross_ref = refs.pop(0) if degree < DEGREE - 1 else None
    fields_ref, extra_ref = refs
    scale = factors_ref[2 * degree][:1]
    carried = factors_ref[2 * degree + 1][:1]
    rows = part_ref.shape[0]
    blocks = []
    for slot in range(2 * REACH):
        offset = slot - REACH if slot < REACH else slot - REACH + 1
        blocks.append(halo_ref[jnp.bitwise_and(place_ref[0] - offset, GROUP - 1)])
    reached = dot(halos_ref[...], jnp.concatenate(blocks, axis=0))
    reached = reached[:TILE] + reached[TILE:]
    for at in range(0, rows, TILE):
        image = part_ref[pl.ds(at, TILE), :]
        if at == rows - TILE:
            image = image + reached
        image = image * scale
        if degree > 0:
            image = image - carried * before_ref[pl.ds(at, TILE), :]
        fields_ref[pl.ds(at, TILE), :] = image
        if degree == DEGREE - 1:
            for copy in range(extra_ref.shape[0]):
                extra_ref[copy, pl.ds(at, TILE), :] = image.astype(BF16)
    if degree < DEGREE - 1:
        extra_ref[...] = dot(cross_ref[...], fields_ref[...].astype(BF16)).astype(BF16)


def end_kernel(scaling, fields_ref, summed_ref, filtered_ref, margin_ref):
    filtered_ref[...] = fields_ref[...]
    margin_ref[...] = summed_ref[...] * scaling


def margin_kernel(band_ref, every_ref, partial_ref):
    bands, _, width = every_ref.shape
    wanted = 2 * bands
    order = [band % 2 * (bands // 2) + band // 2 for band in range(bands)]
    row = lax.broadcasted_iota(jnp.int32, (wanted, width), 0)
    column = lax.broadcasted_iota(jnp.int32, (wanted, width), 1)
    target = jnp.right_shift(row, 1) * wanted + 2 * band_ref[0] + jnp.bitwise_and(row, 1)
    pick = jnp.where(column == target, 1.0, 0.0).astype(BF16)
    chosen = [
        lax.dot_general(pick, every_ref[order[band]], (((1,), (1,)), ((), ())), preferred_element_type=F32).astype(BF16)
        for band in range(bands)
    ]
    chosen = jnp.concatenate(chosen, axis=0)
    for band in range(bands):
        partial_ref[:, pl.ds(band * width, width)] = dot(chosen, every_ref[order[band]]).astype(BF16)


def call(kernel, operands, specs, outs, flops, scratch=()):
    moved = sum(x.size * x.dtype.itemsize for x in (*operands, *outs))
    return pl.pallas_call(
        kernel,
        out_shape=tuple(outs),
        in_specs=specs,
        out_specs=tuple(VMEM for _ in outs),
        scratch_shapes=list(scratch),
        compiler_params=pltpu.CompilerParams(vmem_limit_bytes=16 * 1024 * 1024),
        cost_estimate=pl.CostEstimate(flops=flops, bytes_accessed=moved, transcendentals=0),
    )(*operands)


def shape(dims, dtype=F32):
    return jax.ShapeDtypeStruct(dims, dtype)


def across(crossing, parts):
    route = []
    for at in range(parts):
        place = at % GROUP
        if place >= 5 and at + GROUP < parts:
            route.append((at, at + GROUP))
        if place <= 2 and at >= GROUP:
            route.append((at, at - GROUP))
    return lax.ppermute(crossing, "grid", route)


def exchanged(outgoing, relayed, place, parts):
    zeros = jnp.zeros_like(relayed)
    down = jnp.where(place >= 5, relayed, zeros)
    up = jnp.where(place <= 2, relayed, zeros)
    gap = jnp.zeros((outgoing.shape[0] - 2 * relayed.shape[0], relayed.shape[1]), BF16)
    message = (outgoing + jnp.concatenate([down, gap, up], axis=0)).reshape(GROUP, -1, outgoing.shape[1])
    groups = [list(range(first, first + GROUP)) for first in range(0, parts, GROUP)]
    received = lax.all_to_all(message, "grid", 0, 0, axis_index_groups=groups, tiled=True)
    return received


def on_device(states, potential, bounds, point_count, send_rows, stencil_table):
    rows, width = states.shape
    parts = lax.axis_size("grid")
    bands = lax.axis_size("band")
    slots = GROUP * 64
    place = jnp.bitwise_and(lax.axis_index("grid"), GROUP - 1).reshape(1)
    band = lax.axis_index("band").reshape(1)

    own, cross, crossing = call(
        begin_kernel,
        (place, band, send_rows[0].astype(BF16), states.astype(BF16)),
        [SMEM, SMEM, VMEM, VMEM],
        [shape((slots, rows), BF16), shape((REACH * 64, rows), BF16), shape((REACH * 64, width), BF16)],
        10_000_000,
    )
    relayed = across(crossing, parts)
    high, low, halos, factors, part, outgoing = call(
        build_kernel,
        (bounds.reshape(1, 3), potential.reshape(1, rows), stencil_table, states, own),
        [VMEM] * 5,
        [
            shape((rows, rows), BF16),
            shape((rows, rows), BF16),
            shape((2 * TILE, 2 * REACH * 64), BF16),
            shape((2 * DEGREE, 8, TILE)),
            shape((rows, width)),
            shape((slots, width), BF16),
        ],
        50_000_000,
    )
    before, fields = None, states
    for degree in range(DEGREE):
        if degree > 0:
            relayed = across(extra, parts)
            operands = [fields, high, low, own]
            outs = [shape((rows, width)), shape((slots, width), BF16)]
            if degree == 1:
                before, fields, part, outgoing = call(
                    masking_kernel,
                    [point_count, before] + operands,
                    [SMEM] + [VMEM] * 5,
                    [shape((rows, width))] * 2 + outs,
                    80_000_000,
                )
            else:
                part, outgoing = call(local_kernel, operands, [VMEM] * 4, outs, 80_000_000)
        halo = exchanged(outgoing, relayed, place[0], parts)
        operands = [place, factors, part, halo, halos]
        if degree > 0:
            operands.append(before)
        if degree < DEGREE - 1:
            operands.append(cross)
            after = shape((REACH * 64, width), BF16)
        else:
            after = shape((bands // 2, rows, width), BF16)
        before = fields
        fields, extra = call(
            functools.partial(update_kernel, degree),
            operands,
            [SMEM] + [VMEM] * (len(operands) - 1),
            [shape((rows, width)), after],
            40_000_000,
        )
    alike = [list(range(core, bands, 2)) for core in range(2)]
    chips = [[first, first + 1] for first in range(0, bands, 2)]
    alike_bands = lax.all_to_all(extra, "band", 0, 0, axis_index_groups=alike, tiled=True)
    every_band = lax.all_gather(alike_bands, "band", axis=0, axis_index_groups=chips, tiled=True)
    (partial_sums,) = call(
        margin_kernel,
        (band, every_band),
        [SMEM, VMEM],
        [shape((2 * parts, bands * width), BF16)],
        80_000_000,
    )
    blocks = lax.all_to_all(partial_sums.reshape(parts, 2, bands * width), "grid", 0, 0, tiled=True)
    summed = jnp.sum(blocks.astype(F32), axis=0)
    return call(
        functools.partial(end_kernel, 1.0 / (parts * rows)),
        (fields, summed),
        [VMEM, VMEM],
        [shape((rows, width)), shape(summed.shape)],
        1000,
    )


def solution(mesh):
    placed = (P("grid", "band"), P("grid"), P(), P("grid"), P("grid", None, None), P(None, "grid"))
    return jax.shard_map(
        on_device,
        mesh=mesh,
        in_specs=placed,
        out_specs=(P("grid", "band"), P(("grid", "band"), None)),
        check_vma=False,
    )
```

```python
import functools

import jax
import jax.numpy as jnp
from jax import lax
from jax.experimental import pallas as pl
from jax.experimental.pallas import tpu as pltpu
from jax.sharding import PartitionSpec as P

SPAN = 6
DEGREE = 3
REACH = 3
GROUP = 8

DIFFERENCE_WEIGHTS = (
    -5369.0 / 1800.0,
    12.0 / 7.0,
    -15.0 / 56.0,
    10.0 / 189.0,
    -1.0 / 112.0,
    2.0 / 1925.0,
    -1.0 / 16632.0,
)
KINETIC_SCALE = 0.5 / 0.49
CENTRE_WEIGHT = -3.0 * KINETIC_SCALE * DIFFERENCE_WEIGHTS[0]
TILE = 128
BF16 = jnp.bfloat16
F32 = jnp.float32
VMEM = pl.BlockSpec(memory_space=pltpu.VMEM)
SMEM = pl.BlockSpec(memory_space=pltpu.SMEM)


def dot(a, b):
    return jnp.dot(a, b, preferred_element_type=F32)


def split(values):
    high = values.astype(BF16)
    return high, (values - high.astype(F32)).astype(BF16)


def select_rows(select_ref, sends_ref, offsets, rows):
    sends = sends_ref[...].astype(F32).astype(jnp.int32)

    def block(offset):
        picks = jnp.full((1, 64), rows, jnp.int32)
        for slot in range(2 * REACH):
            kept = slot - REACH if slot < REACH else slot - REACH + 1
            picks = jnp.where(offset == kept, sends[slot : slot + 1, :], picks)
        return picks

    for pair in range((len(offsets) + 1) // 2):
        two = [block(offset) for offset in offsets[2 * pair : 2 * pair + 2]]
        height = 64 * len(two)
        picks = jnp.concatenate([two[0], two[-1]], axis=1)
        for at in range(0, rows, TILE):
            here = lax.broadcasted_iota(jnp.int32, (TILE, TILE), 0) + at
            hit = jnp.where(here == picks, 1.0, 0.0)
            select_ref[pl.ds(pair * TILE, height), pl.ds(at, TILE)] = jnp.transpose(hit)[:height].astype(BF16)


def begin_kernel(
    place_ref, band_ref, sends_ref, states_ref, own_ref, cross_ref, crossing_ref
):
    place = place_ref[0]
    rows = states_ref.shape[0]
    first = jnp.where(place >= 5, GROUP - place, -REACH - place)
    select_rows(cross_ref, sends_ref, [first + at for at in range(REACH)], rows)
    crossing_ref[...] = dot(cross_ref[...], states_ref[...]).astype(BF16)
    select_rows(own_ref, sends_ref, [at - place for at in range(GROUP)], rows)


def local_part(fields, high_ref, low_ref, own_ref, part_ref, outgoing_ref):
    high, low = split(fields)
    part_ref[...] = dot(high_ref[...], high) + dot(low_ref[...], high) + dot(high_ref[...], low)
    outgoing_ref[...] = dot(own_ref[...], high).astype(BF16)


def build_kernel(
    bounds_ref, potential_ref, table_ref, states_ref, own_ref, cross_ref,
    high_ref, low_ref, halos_ref, factors_ref, part_ref, outgoing_ref, reach_ref, base_ref
):
    rows = states_ref.shape[0]
    stencil = table_ref.shape[0]
    lower, cutoff, upper = (jnp.broadcast_to(bounds_ref[:, at : at + 1], (8, TILE)) for at in range(3))
    half = (upper - cutoff) / 2.0
    middle = (upper + cutoff) / 2.0
    sigma = half / (lower - middle)
    twice = 2.0 / sigma
    factors_ref[0] = sigma / half
    factors_ref[1] = jnp.zeros_like(sigma)
    for degree in range(1, DEGREE):
        following = 1.0 / (twice - sigma)
        factors_ref[2 * degree] = 2.0 * following / half
        factors_ref[2 * degree + 1] = sigma * following
        sigma = following
    middle = middle[:1]
    def gathered(column, row):
        here = lax.broadcasted_iota(jnp.int32, (TILE, TILE), 0) + column
        total = jnp.zeros((TILE, TILE), F32)
        for neighbour in range(stencil):
            weight = -KINETIC_SCALE * DIFFERENCE_WEIGHTS[neighbour % SPAN + 1]
            names = table_ref[neighbour : neighbour + 1, row : row + TILE]
            total = total + jnp.where(here == names, weight, 0.0)
        return total, here

    for row in range(0, rows, TILE):
        diagonal = potential_ref[:, row : row + TILE] + (CENTRE_WEIGHT - middle)

        @pl.loop(0, rows // TILE)
        def _(block, row=row, diagonal=diagonal):
            column = pl.multiple_of(block * TILE, TILE)
            total, here = gathered(column, row)
            right = lax.broadcasted_iota(jnp.int32, (TILE, TILE), 1) + row
            total = total + jnp.where(here == right, diagonal, 0.0)
            high, low = split(jnp.transpose(total))
            high_ref[pl.ds(row, TILE), pl.ds(column, TILE)] = high
            low_ref[pl.ds(row, TILE), pl.ds(column, TILE)] = low

    @pl.loop(0, 2 * REACH * 64 // TILE)
    def _(block):
        column = pl.multiple_of(block * TILE, TILE)
        total, _ = gathered(column + rows + 1, rows - TILE)
        high, low = split(jnp.transpose(total))
        halos_ref[pl.ds(0, TILE), pl.ds(column, TILE)] = high
        halos_ref[pl.ds(TILE, TILE), pl.ds(column, TILE)] = low

    local_part(states_ref[...], high_ref, low_ref, own_ref, part_ref, outgoing_ref)
    crossing = cross_ref.shape[0]
    for at in range(2):
        named = dot(cross_ref[:, rows - TILE :], halos_ref[pl.ds(at * TILE, TILE), :])
        reach_ref[pl.ds(at * crossing, crossing), :] = named.astype(BF16)
    base_ref[...] = selected(cross_ref, part_ref[...] * factors_ref[0][:1])


def selected(select_ref, values):
    high, low = split(values)
    return dot(select_ref[...], high) + dot(select_ref[...], low)


def in_order(place_ref, halo_ref):
    blocks = []
    for slot in range(2 * REACH):
        offset = slot - REACH if slot < REACH else slot - REACH + 1
        blocks.append(halo_ref[jnp.bitwise_and(place_ref[0] - offset, GROUP - 1)])
    return jnp.concatenate(blocks, axis=0)


def crossing_kernel(degree, place_ref, factors_ref, base_ref, halo_ref, reach_ref, crossing_ref):
    rows = crossing_ref.shape[0]
    reached = dot(reach_ref[...], in_order(place_ref, halo_ref))
    reached = (reached[:rows] + reached[rows:]) * factors_ref[2 * degree][:1]
    crossing_ref[...] = (base_ref[...] + reached).astype(BF16)


def updated(degree, place_ref, factors_ref, part_ref, halo_ref, halos_ref, before_ref):
    rows = part_ref.shape[0]
    reached = dot(halos_ref[...], in_order(place_ref, halo_ref))
    reached = reached[:TILE] + reached[TILE:]
    image = jnp.concatenate([part_ref[pl.ds(0, rows - TILE), :], part_ref[pl.ds(rows - TILE, TILE), :] + reached], axis=0)
    image = image * factors_ref[2 * degree][:1]
    if degree > 0:
        image = image - factors_ref[2 * degree + 1][:1] * before_ref[...]
    return image


def first_kernel(
    place_ref, count_ref, factors_ref, old_ref, halo_ref, halos_ref, states_ref, high_ref, low_ref, own_ref, cross_ref,
    fields_ref, part_ref, outgoing_ref, start_ref, base_ref
):
    live = lax.broadcasted_iota(jnp.int32, states_ref.shape, 0) < count_ref[0]
    start_ref[...] = jnp.where(live, states_ref[...], 0.0)
    fields_ref[...] = jnp.where(live, updated(0, place_ref, factors_ref, old_ref, halo_ref, halos_ref, None), 0.0)
    local_part(fields_ref[...], high_ref, low_ref, own_ref, part_ref, outgoing_ref)
    base_ref[...] = selected(
        cross_ref, part_ref[...] * factors_ref[2][:1] - factors_ref[3][:1] * start_ref[...]
    )


def second_kernel(
    place_ref, factors_ref, old_ref, halo_ref, halos_ref, start_ref, high_ref, low_ref, own_ref,
    fields_ref, part_ref, outgoing_ref
):
    fields_ref[...] = updated(1, place_ref, factors_ref, old_ref, halo_ref, halos_ref, start_ref)
    local_part(fields_ref[...], high_ref, low_ref, own_ref, part_ref, outgoing_ref)


def last_kernel(place_ref, factors_ref, part_ref, halo_ref, halos_ref, before_ref, fields_ref, copies_ref):
    fields_ref[...] = updated(2, place_ref, factors_ref, part_ref, halo_ref, halos_ref, before_ref)
    for copy in range(copies_ref.shape[0]):
        copies_ref[copy] = fields_ref[...].astype(BF16)


def end_kernel(scaling, fields_ref, summed_ref, filtered_ref, margin_ref):
    filtered_ref[...] = fields_ref[...]
    margin_ref[...] = summed_ref[...] * scaling


def margin_kernel(band_ref, every_ref, partial_ref):
    bands, _, width = every_ref.shape
    wanted = 2 * bands
    order = [band % 2 * (bands // 2) + band // 2 for band in range(bands)]
    row = lax.broadcasted_iota(jnp.int32, (wanted, width), 0)
    column = lax.broadcasted_iota(jnp.int32, (wanted, width), 1)
    target = jnp.right_shift(row, 1) * wanted + 2 * band_ref[0] + jnp.bitwise_and(row, 1)
    pick = jnp.where(column == target, 1.0, 0.0).astype(BF16)
    chosen = [
        lax.dot_general(pick, every_ref[order[band]], (((1,), (1,)), ((), ())), preferred_element_type=F32).astype(BF16)
        for band in range(bands)
    ]
    chosen = jnp.concatenate(chosen, axis=0)
    for band in range(bands):
        partial_ref[:, pl.ds(band * width, width)] = dot(chosen, every_ref[order[band]]).astype(BF16)


def call(kernel, operands, specs, outs, flops, scratch=()):
    moved = sum(x.size * x.dtype.itemsize for x in (*operands, *outs))
    return pl.pallas_call(
        kernel,
        out_shape=tuple(outs),
        in_specs=specs,
        out_specs=tuple(VMEM for _ in outs),
        scratch_shapes=list(scratch),
        compiler_params=pltpu.CompilerParams(vmem_limit_bytes=16 * 1024 * 1024),
        cost_estimate=pl.CostEstimate(flops=flops, bytes_accessed=moved, transcendentals=0),
    )(*operands)


def shape(dims, dtype=F32):
    return jax.ShapeDtypeStruct(dims, dtype)


def across(crossing, parts):
    route = []
    for at in range(parts):
        place = at % GROUP
        if place >= 5 and at + GROUP < parts:
            route.append((at, at + GROUP))
        if place <= 2 and at >= GROUP:
            route.append((at, at - GROUP))
    return lax.ppermute(crossing, "grid", route)


def exchanged(outgoing, relayed, place, parts):
    zeros = jnp.zeros_like(relayed)
    down = jnp.where(place >= 5, relayed, zeros)
    up = jnp.where(place <= 2, relayed, zeros)
    gap = jnp.zeros((outgoing.shape[0] - 2 * relayed.shape[0], relayed.shape[1]), BF16)
    message = (outgoing + jnp.concatenate([down, gap, up], axis=0)).reshape(GROUP, -1, outgoing.shape[1])
    groups = [list(range(first, first + GROUP)) for first in range(0, parts, GROUP)]
    received = lax.all_to_all(message, "grid", 0, 0, axis_index_groups=groups, tiled=True)
    return received


def on_device(states, potential, bounds, point_count, send_rows, stencil_table):
    rows, width = states.shape
    parts = lax.axis_size("grid")
    bands = lax.axis_size("band")
    slots = GROUP * 64
    place = jnp.bitwise_and(lax.axis_index("grid"), GROUP - 1).reshape(1)
    band = lax.axis_index("band").reshape(1)

    rounded, send_rows = lax.optimization_barrier((states.astype(BF16), send_rows))
    own, cross, crossing = call(
        begin_kernel,
        (place, band, send_rows[0].astype(BF16), rounded),
        [SMEM, SMEM, VMEM, VMEM],
        [shape((slots, rows), BF16), shape((REACH * 64, rows), BF16), shape((REACH * 64, width), BF16)],
        10_000_000,
    )
    relayed = across(crossing, parts)
    high, low, halos, factors, part, outgoing, reach, base = call(
        build_kernel,
        (bounds.reshape(1, 3), potential.reshape(1, rows), stencil_table, states, own, cross),
        [VMEM] * 6,
        [
            shape((rows, rows), BF16),
            shape((rows, rows), BF16),
            shape((2 * TILE, 2 * REACH * 64), BF16),
            shape((2 * DEGREE, 8, TILE)),
            shape((rows, width)),
            shape((slots, width), BF16),
            shape((2 * REACH * 64, 2 * REACH * 64), BF16),
            shape((REACH * 64, width)),
        ],
        50_000_000,
    )
    square = shape((rows, width))
    outs = [square, square, shape((slots, width), BF16)]

    def crossed(degree, base, halo):
        (crossing,) = call(
            functools.partial(crossing_kernel, degree),
            (place, factors, base, halo, reach),
            [SMEM] + [VMEM] * 4,
            [shape((REACH * 64, width), BF16)],
            40_000_000,
        )
        return across(crossing, parts)

    halo = exchanged(outgoing, relayed, place[0], parts)
    relayed = crossed(0, base, halo)
    first, part, outgoing, start, base = call(
        first_kernel,
        (place, point_count, factors, part, halo, halos, states, high, low, own, cross),
        [SMEM, SMEM] + [VMEM] * 9,
        outs + [square, shape((REACH * 64, width))],
        80_000_000,
    )
    halo = exchanged(outgoing, relayed, place[0], parts)
    relayed = crossed(1, base, halo)
    second, part, outgoing = call(
        second_kernel,
        (place, factors, part, halo, halos, start, high, low, own),
        [SMEM] + [VMEM] * 8,
        outs,
        80_000_000,
    )
    halo = exchanged(outgoing, relayed, place[0], parts)
    fields, extra = call(
        last_kernel,
        (place, factors, part, halo, halos, first),
        [SMEM] + [VMEM] * 5,
        [square, shape((bands // 2, rows, width), BF16)],
        40_000_000,
    )
    alike = [list(range(core, bands, 2)) for core in range(2)]
    chips = [[first, first + 1] for first in range(0, bands, 2)]
    alike_bands = lax.all_to_all(extra, "band", 0, 0, axis_index_groups=alike, tiled=True)
    every_band = lax.all_gather(alike_bands, "band", axis=0, axis_index_groups=chips, tiled=True)
    (partial_sums,) = call(
        margin_kernel,
        (band, every_band),
        [SMEM, VMEM],
        [shape((2 * parts, bands * width), BF16)],
        80_000_000,
    )
    blocks = lax.all_to_all(partial_sums.reshape(parts, 2, bands * width), "grid", 0, 0, tiled=True)
    summed = jnp.sum(blocks.astype(F32), axis=0)
    return call(
        functools.partial(end_kernel, 1.0 / (parts * rows)),
        (fields, summed),
        [VMEM, VMEM],
        [shape((rows, width)), shape(summed.shape)],
        1000,
    )


def solution(mesh):
    placed = (P("grid", "band"), P("grid"), P(), P("grid"), P("grid", None, None), P(None, "grid"))
    return jax.shard_map(
        on_device,
        mesh=mesh,
        in_specs=placed,
        out_specs=(P("grid", "band"), P(("grid", "band"), None)),
        check_vma=False,
    )
```

```python
import functools

import jax
import jax.numpy as jnp
from jax import lax
from jax.experimental import pallas as pl
from jax.experimental.pallas import tpu as pltpu
from jax.sharding import PartitionSpec as P

SPAN = 6
DEGREE = 3
REACH = 3
GROUP = 8

DIFFERENCE_WEIGHTS = (
    -5369.0 / 1800.0,
    12.0 / 7.0,
    -15.0 / 56.0,
    10.0 / 189.0,
    -1.0 / 112.0,
    2.0 / 1925.0,
    -1.0 / 16632.0,
)
KINETIC_SCALE = 0.5 / 0.49
CENTRE_WEIGHT = -3.0 * KINETIC_SCALE * DIFFERENCE_WEIGHTS[0]
TILE = 128
BF16 = jnp.bfloat16
F32 = jnp.float32
VMEM = pl.BlockSpec(memory_space=pltpu.VMEM)
SMEM = pl.BlockSpec(memory_space=pltpu.SMEM)


def dot(a, b):
    return jnp.dot(a, b, preferred_element_type=F32)


def split(values):
    high = values.astype(BF16)
    return high, (values - high.astype(F32)).astype(BF16)


def select_rows(select_ref, sends_ref, offsets, rows):
    sends = sends_ref[...].astype(F32).astype(jnp.int32)

    def block(offset):
        picks = jnp.full((1, 64), rows, jnp.int32)
        for slot in range(2 * REACH):
            kept = slot - REACH if slot < REACH else slot - REACH + 1
            picks = jnp.where(offset == kept, sends[slot : slot + 1, :], picks)
        return picks

    for pair in range((len(offsets) + 1) // 2):
        two = [block(offset) for offset in offsets[2 * pair : 2 * pair + 2]]
        height = 64 * len(two)
        picks = jnp.concatenate([two[0], two[-1]], axis=1)
        for at in range(0, rows, TILE):
            here = lax.broadcasted_iota(jnp.int32, (TILE, TILE), 0) + at
            hit = jnp.where(here == picks, 1.0, 0.0)
            select_ref[pl.ds(pair * TILE, height), pl.ds(at, TILE)] = jnp.transpose(hit)[:height].astype(BF16)


def begin_kernel(
    place_ref, band_ref, sends_ref, states_ref, own_ref, cross_ref, crossing_ref
):
    place = place_ref[0]
    rows = states_ref.shape[0]
    first = jnp.where(place >= 5, GROUP - place, -REACH - place)
    select_rows(cross_ref, sends_ref, [first + at for at in range(REACH)], rows)
    crossing_ref[...] = dot(cross_ref[...], states_ref[...]).astype(BF16)
    select_rows(own_ref, sends_ref, [at - place for at in range(GROUP)], rows)


def local_part(fields, high_ref, low_ref, own_ref, part_ref, outgoing_ref):
    high, low = split(fields)
    part_ref[...] = dot(high_ref[...], high) + dot(low_ref[...], high) + dot(high_ref[...], low)
    outgoing_ref[...] = dot(own_ref[...], high).astype(BF16)


def build_kernel(
    bounds_ref, potential_ref, table_ref, states_ref, own_ref, cross_ref,
    high_ref, low_ref, halos_ref, factors_ref, part_ref, outgoing_ref, reach_ref, base_ref
):
    rows = states_ref.shape[0]
    stencil = table_ref.shape[0]
    lower, cutoff, upper = (jnp.broadcast_to(bounds_ref[:, at : at + 1], (8, TILE)) for at in range(3))
    half = (upper - cutoff) / 2.0
    middle = (upper + cutoff) / 2.0
    sigma = half / (lower - middle)
    twice = 2.0 / sigma
    factors_ref[0] = sigma / half
    factors_ref[1] = jnp.zeros_like(sigma)
    for degree in range(1, DEGREE):
        following = 1.0 / (twice - sigma)
        factors_ref[2 * degree] = 2.0 * following / half
        factors_ref[2 * degree + 1] = sigma * following
        sigma = following
    middle = middle[:1]
    def gathered(column, row):
        here = lax.broadcasted_iota(jnp.int32, (TILE, TILE), 0) + column
        total = jnp.zeros((TILE, TILE), F32)
        for neighbour in range(stencil):
            weight = -KINETIC_SCALE * DIFFERENCE_WEIGHTS[neighbour % SPAN + 1]
            names = table_ref[neighbour : neighbour + 1, row : row + TILE]
            total = total + jnp.where(here == names, weight, 0.0)
        return total, here

    for row in range(0, rows, TILE):
        diagonal = potential_ref[:, row : row + TILE] + (CENTRE_WEIGHT - middle)

        @pl.loop(0, rows // TILE)
        def _(block, row=row, diagonal=diagonal):
            column = pl.multiple_of(block * TILE, TILE)
            total, here = gathered(column, row)
            right = lax.broadcasted_iota(jnp.int32, (TILE, TILE), 1) + row
            total = total + jnp.where(here == right, diagonal, 0.0)
            high, low = split(jnp.transpose(total))
            high_ref[pl.ds(row, TILE), pl.ds(column, TILE)] = high
            low_ref[pl.ds(row, TILE), pl.ds(column, TILE)] = low

    @pl.loop(0, 2 * REACH * 64 // TILE)
    def _(block):
        column = pl.multiple_of(block * TILE, TILE)
        total, _ = gathered(column + rows + 1, rows - TILE)
        high, low = split(jnp.transpose(total))
        halos_ref[pl.ds(0, TILE), pl.ds(column, TILE)] = high
        halos_ref[pl.ds(TILE, TILE), pl.ds(column, TILE)] = low

    local_part(states_ref[...], high_ref, low_ref, own_ref, part_ref, outgoing_ref)
    crossing = cross_ref.shape[0]
    for at in range(2):
        named = dot(cross_ref[:, rows - TILE :], halos_ref[pl.ds(at * TILE, TILE), :])
        reach_ref[pl.ds(at * crossing, crossing), :] = named.astype(BF16)
    base_ref[...] = selected(cross_ref, part_ref[...] * factors_ref[0][:1])


def selected(select_ref, values):
    high, low = split(values)
    return dot(select_ref[...], high) + dot(select_ref[...], low)


def in_order(place_ref, halo_ref):
    blocks = []
    for slot in range(2 * REACH):
        offset = slot - REACH if slot < REACH else slot - REACH + 1
        blocks.append(halo_ref[jnp.bitwise_and(place_ref[0] - offset, GROUP - 1)])
    return jnp.concatenate(blocks, axis=0)


def crossing_kernel(degree, place_ref, factors_ref, base_ref, halo_ref, reach_ref, crossing_ref):
    rows = crossing_ref.shape[0]
    reached = dot(reach_ref[...], in_order(place_ref, halo_ref))
    reached = (reached[:rows] + reached[rows:]) * factors_ref[2 * degree][:1]
    crossing_ref[...] = (base_ref[...] + reached).astype(BF16)


def updated(degree, place_ref, factors_ref, part_ref, halo_ref, halos_ref, before_ref):
    rows = part_ref.shape[0]
    reached = dot(halos_ref[...], in_order(place_ref, halo_ref))
    reached = reached[:TILE] + reached[TILE:]
    image = jnp.concatenate([part_ref[pl.ds(0, rows - TILE), :], part_ref[pl.ds(rows - TILE, TILE), :] + reached], axis=0)
    image = image * factors_ref[2 * degree][:1]
    if degree > 0:
        image = image - factors_ref[2 * degree + 1][:1] * before_ref[...]
    return image


def first_kernel(
    place_ref, count_ref, factors_ref, old_ref, halo_ref, halos_ref, states_ref, high_ref, low_ref, own_ref, cross_ref,
    fields_ref, part_ref, outgoing_ref, start_ref, base_ref
):
    live = lax.broadcasted_iota(jnp.int32, states_ref.shape, 0) < count_ref[0]
    start_ref[...] = jnp.where(live, states_ref[...], 0.0)
    fields_ref[...] = jnp.where(live, updated(0, place_ref, factors_ref, old_ref, halo_ref, halos_ref, None), 0.0)
    local_part(fields_ref[...], high_ref, low_ref, own_ref, part_ref, outgoing_ref)
    base_ref[...] = selected(
        cross_ref, part_ref[...] * factors_ref[2][:1] - factors_ref[3][:1] * start_ref[...]
    )


def second_kernel(
    place_ref, factors_ref, old_ref, halo_ref, halos_ref, start_ref, high_ref, low_ref, own_ref,
    fields_ref, part_ref, outgoing_ref
):
    fields_ref[...] = updated(1, place_ref, factors_ref, old_ref, halo_ref, halos_ref, start_ref)
    local_part(fields_ref[...], high_ref, low_ref, own_ref, part_ref, outgoing_ref)


def last_kernel(place_ref, factors_ref, part_ref, halo_ref, halos_ref, before_ref, fields_ref, copies_ref):
    fields_ref[...] = updated(2, place_ref, factors_ref, part_ref, halo_ref, halos_ref, before_ref)
    for copy in range(copies_ref.shape[0]):
        copies_ref[copy] = fields_ref[...].astype(BF16)


def end_kernel(scaling, fields_ref, summed_ref, filtered_ref, margin_ref):
    filtered_ref[...] = fields_ref[...]
    margin_ref[...] = summed_ref[...] * scaling


def margin_kernel(band_ref, every_ref, partial_ref):
    bands, _, width = every_ref.shape
    wanted = 2 * bands
    order = [band % 2 * (bands // 2) + band // 2 for band in range(bands)]
    row = lax.broadcasted_iota(jnp.int32, (wanted, width), 0)
    column = lax.broadcasted_iota(jnp.int32, (wanted, width), 1)
    target = (bands - 1 - jnp.right_shift(row, 1)) * wanted + 2 * band_ref[0] + jnp.bitwise_and(row, 1)
    pick = jnp.where(column == target, 1.0, 0.0).astype(BF16)
    chosen = [
        lax.dot_general(pick, every_ref[order[band]], (((1,), (1,)), ((), ())), preferred_element_type=F32).astype(BF16)
        for band in reversed(range(bands))
    ]
    chosen = jnp.concatenate(chosen, axis=0)
    for band in range(0, bands, 2):
        both = jnp.concatenate([every_ref[order[band]], every_ref[order[band + 1]]], axis=1)
        partial_ref[:, pl.ds(band * width, 2 * width)] = dot(chosen, both).astype(BF16)


def call(kernel, operands, specs, outs, flops, scratch=()):
    moved = sum(x.size * x.dtype.itemsize for x in (*operands, *outs))
    return pl.pallas_call(
        kernel,
        out_shape=tuple(outs),
        in_specs=specs,
        out_specs=tuple(VMEM for _ in outs),
        scratch_shapes=list(scratch),
        compiler_params=pltpu.CompilerParams(vmem_limit_bytes=16 * 1024 * 1024),
        cost_estimate=pl.CostEstimate(flops=flops, bytes_accessed=moved, transcendentals=0),
    )(*operands)


def shape(dims, dtype=F32):
    return jax.ShapeDtypeStruct(dims, dtype)


def across(crossing, parts):
    route = []
    for at in range(parts):
        place = at % GROUP
        if place >= 5 and at + GROUP < parts:
            route.append((at, at + GROUP))
        if place <= 2 and at >= GROUP:
            route.append((at, at - GROUP))
    return lax.ppermute(crossing, "grid", route)


def exchanged(outgoing, relayed, place, parts):
    zeros = jnp.zeros_like(relayed)
    down = jnp.where(place >= 5, relayed, zeros)
    up = jnp.where(place <= 2, relayed, zeros)
    gap = jnp.zeros((outgoing.shape[0] - 2 * relayed.shape[0], relayed.shape[1]), BF16)
    message = (outgoing + jnp.concatenate([down, gap, up], axis=0)).reshape(GROUP, -1, outgoing.shape[1])
    groups = [list(range(first, first + GROUP)) for first in range(0, parts, GROUP)]
    received = lax.all_to_all(message, "grid", 0, 0, axis_index_groups=groups, tiled=True)
    return received


def on_device(states, potential, bounds, point_count, send_rows, stencil_table):
    rows, width = states.shape
    parts = lax.axis_size("grid")
    bands = lax.axis_size("band")
    slots = GROUP * 64
    place = jnp.bitwise_and(lax.axis_index("grid"), GROUP - 1).reshape(1)
    band = lax.axis_index("band").reshape(1)

    rounded, send_rows = lax.optimization_barrier((states.astype(BF16), send_rows))
    own, cross, crossing = call(
        begin_kernel,
        (place, band, send_rows[0].astype(BF16), rounded),
        [SMEM, SMEM, VMEM, VMEM],
        [shape((slots, rows), BF16), shape((REACH * 64, rows), BF16), shape((REACH * 64, width), BF16)],
        10_000_000,
    )
    relayed = across(crossing, parts)
    high, low, halos, factors, part, outgoing, reach, base = call(
        build_kernel,
        (bounds.reshape(1, 3), potential.reshape(1, rows), stencil_table, states, own, cross),
        [VMEM] * 6,
        [
            shape((rows, rows), BF16),
            shape((rows, rows), BF16),
            shape((2 * TILE, 2 * REACH * 64), BF16),
            shape((2 * DEGREE, 8, TILE)),
            shape((rows, width)),
            shape((slots, width), BF16),
            shape((2 * REACH * 64, 2 * REACH * 64), BF16),
            shape((REACH * 64, width)),
        ],
        50_000_000,
    )
    square = shape((rows, width))
    outs = [square, square, shape((slots, width), BF16)]

    def crossed(degree, base, halo):
        (crossing,) = call(
            functools.partial(crossing_kernel, degree),
            (place, factors, base, halo, reach),
            [SMEM] + [VMEM] * 4,
            [shape((REACH * 64, width), BF16)],
            40_000_000,
        )
        return across(crossing, parts)

    halo = exchanged(outgoing, relayed, place[0], parts)
    relayed = crossed(0, base, halo)
    first, part, outgoing, start, base = call(
        first_kernel,
        (place, point_count, factors, part, halo, halos, states, high, low, own, cross),
        [SMEM, SMEM] + [VMEM] * 9,
        outs + [square, shape((REACH * 64, width))],
        80_000_000,
    )
    halo = exchanged(outgoing, relayed, place[0], parts)
    relayed = crossed(1, base, halo)
    second, part, outgoing = call(
        second_kernel,
        (place, factors, part, halo, halos, start, high, low, own),
        [SMEM] + [VMEM] * 8,
        outs,
        80_000_000,
    )
    halo = exchanged(outgoing, relayed, place[0], parts)
    fields, extra = call(
        last_kernel,
        (place, factors, part, halo, halos, first),
        [SMEM] + [VMEM] * 5,
        [square, shape((bands // 2, rows, width), BF16)],
        40_000_000,
    )
    alike = [list(range(core, bands, 2)) for core in range(2)]
    chips = [[first, first + 1] for first in range(0, bands, 2)]
    alike_bands = lax.all_to_all(extra, "band", 0, 0, axis_index_groups=alike, tiled=True)
    every_band = lax.all_gather(alike_bands, "band", axis=0, axis_index_groups=chips, tiled=True)
    (partial_sums,) = call(
        margin_kernel,
        (band, every_band),
        [SMEM, VMEM],
        [shape((2 * parts, bands * width), BF16)],
        80_000_000,
    )
    blocks = lax.all_to_all(
        partial_sums.reshape(parts, 2, bands * width),
        "grid",
        0,
        0,
        axis_index_groups=[list(reversed(range(parts)))],
        tiled=True,
    )
    summed = jnp.sum(blocks.astype(F32), axis=0)
    return call(
        functools.partial(end_kernel, 1.0 / (parts * rows)),
        (fields, summed),
        [VMEM, VMEM],
        [shape((rows, width)), shape(summed.shape)],
        1000,
    )


def solution(mesh):
    placed = (P("grid", "band"), P("grid"), P(), P("grid"), P("grid", None, None), P(None, "grid"))
    return jax.shard_map(
        on_device,
        mesh=mesh,
        in_specs=placed,
        out_specs=(P("grid", "band"), P(("grid", "band"), None)),
        check_vma=False,
    )
```

```python
import functools

import jax
import jax.numpy as jnp
from jax import lax
from jax.experimental import pallas as pl
from jax.experimental.pallas import tpu as pltpu
from jax.sharding import PartitionSpec as P

SPAN = 6
DEGREE = 3
REACH = 3
GROUP = 8

DIFFERENCE_WEIGHTS = (
    -5369.0 / 1800.0,
    12.0 / 7.0,
    -15.0 / 56.0,
    10.0 / 189.0,
    -1.0 / 112.0,
    2.0 / 1925.0,
    -1.0 / 16632.0,
)
KINETIC_SCALE = 0.5 / 0.49
CENTRE_WEIGHT = -3.0 * KINETIC_SCALE * DIFFERENCE_WEIGHTS[0]
TILE = 128
BF16 = jnp.bfloat16
F32 = jnp.float32
VMEM = pl.BlockSpec(memory_space=pltpu.VMEM)
SMEM = pl.BlockSpec(memory_space=pltpu.SMEM)


def dot(a, b):
    return jnp.dot(a, b, preferred_element_type=F32)


def split(values):
    high = values.astype(BF16)
    return high, (values - high.astype(F32)).astype(BF16)


def select_rows(select_ref, sends_ref, offsets, rows):
    sends = sends_ref[...].astype(F32).astype(jnp.int32)

    def block(offset):
        picks = jnp.full((1, 64), rows, jnp.int32)
        for slot in range(2 * REACH):
            kept = slot - REACH if slot < REACH else slot - REACH + 1
            picks = jnp.where(offset == kept, sends[slot : slot + 1, :], picks)
        return picks

    for pair in range((len(offsets) + 1) // 2):
        two = [block(offset) for offset in offsets[2 * pair : 2 * pair + 2]]
        height = 64 * len(two)
        picks = jnp.concatenate([two[0], two[-1]], axis=1)
        for at in range(0, rows, TILE):
            here = lax.broadcasted_iota(jnp.int32, (TILE, TILE), 0) + at
            hit = jnp.where(here == picks, 1.0, 0.0)
            select_ref[pl.ds(pair * TILE, height), pl.ds(at, TILE)] = jnp.transpose(hit)[:height].astype(BF16)


def begin_kernel(
    place_ref, band_ref, sends_ref, states_ref, cross_ref, crossing_ref
):
    place = place_ref[0]
    rows = states_ref.shape[0]
    first = jnp.where(place >= 5, GROUP - place, -REACH - place)
    select_rows(cross_ref, sends_ref, [first + at for at in range(REACH)], rows)
    crossing_ref[...] = dot(cross_ref[...], states_ref[...]).astype(BF16)


def local_part(fields, high_ref, low_ref, own_ref, part_ref, outgoing_ref):
    high, low = split(fields)
    part_ref[...] = dot(high_ref[...], high) + dot(low_ref[...], high) + dot(high_ref[...], low)
    outgoing_ref[...] = dot(own_ref[...], high).astype(BF16)


def build_kernel(
    place_ref, bounds_ref, potential_ref, table_ref, states_ref, sends_ref, cross_ref, own_ref,
    high_ref, low_ref, halos_ref, factors_ref, part_ref, outgoing_ref, reach_ref, base_ref
):
    rows = states_ref.shape[0]
    stencil = table_ref.shape[0]
    lower, cutoff, upper = (jnp.broadcast_to(bounds_ref[:, at : at + 1], (8, TILE)) for at in range(3))
    half = (upper - cutoff) / 2.0
    middle = (upper + cutoff) / 2.0
    sigma = half / (lower - middle)
    twice = 2.0 / sigma
    factors_ref[0] = sigma / half
    factors_ref[1] = jnp.zeros_like(sigma)
    for degree in range(1, DEGREE):
        following = 1.0 / (twice - sigma)
        factors_ref[2 * degree] = 2.0 * following / half
        factors_ref[2 * degree + 1] = sigma * following
        sigma = following
    middle = middle[:1]
    def gathered(column, row):
        here = lax.broadcasted_iota(jnp.int32, (TILE, TILE), 0) + column
        total = jnp.zeros((TILE, TILE), F32)
        for neighbour in range(stencil):
            weight = -KINETIC_SCALE * DIFFERENCE_WEIGHTS[neighbour % SPAN + 1]
            names = table_ref[neighbour : neighbour + 1, row : row + TILE]
            total = total + jnp.where(here == names, weight, 0.0)
        return total, here

    for row in range(0, rows, TILE):
        diagonal = potential_ref[:, row : row + TILE] + (CENTRE_WEIGHT - middle)

        @pl.loop(0, rows // TILE)
        def _(block, row=row, diagonal=diagonal):
            column = pl.multiple_of(block * TILE, TILE)
            total, here = gathered(column, row)
            right = lax.broadcasted_iota(jnp.int32, (TILE, TILE), 1) + row
            total = total + jnp.where(here == right, diagonal, 0.0)
            high, low = split(jnp.transpose(total))
            high_ref[pl.ds(row, TILE), pl.ds(column, TILE)] = high
            low_ref[pl.ds(row, TILE), pl.ds(column, TILE)] = low

    @pl.loop(0, 2 * REACH * 64 // TILE)
    def _(block):
        column = pl.multiple_of(block * TILE, TILE)
        total, _ = gathered(column + rows + 1, rows - TILE)
        high, low = split(jnp.transpose(total))
        halos_ref[pl.ds(0, TILE), pl.ds(column, TILE)] = high
        halos_ref[pl.ds(TILE, TILE), pl.ds(column, TILE)] = low

    select_rows(own_ref, sends_ref, [at - place_ref[0] for at in range(GROUP)], rows)
    local_part(states_ref[...], high_ref, low_ref, own_ref, part_ref, outgoing_ref)
    crossing = cross_ref.shape[0]
    for at in range(2):
        named = dot(cross_ref[:, rows - TILE :], halos_ref[pl.ds(at * TILE, TILE), :])
        reach_ref[pl.ds(at * crossing, crossing), :] = named.astype(BF16)
    base_ref[...] = selected(cross_ref, part_ref[...] * factors_ref[0][:1])


def selected(select_ref, values):
    high, low = split(values)
    return dot(select_ref[...], high) + dot(select_ref[...], low)


def in_order(place_ref, halo_ref):
    blocks = []
    for slot in range(2 * REACH):
        offset = slot - REACH if slot < REACH else slot - REACH + 1
        blocks.append(halo_ref[jnp.bitwise_and(place_ref[0] - offset, GROUP - 1)])
    return jnp.concatenate(blocks, axis=0)


def crossing_kernel(degree, place_ref, factors_ref, base_ref, halo_ref, reach_ref, crossing_ref):
    rows = crossing_ref.shape[0]
    reached = dot(reach_ref[...], in_order(place_ref, halo_ref))
    reached = (reached[:rows] + reached[rows:]) * factors_ref[2 * degree][:1]
    crossing_ref[...] = (base_ref[...] + reached).astype(BF16)


def updated(degree, place_ref, factors_ref, part_ref, halo_ref, halos_ref, before_ref):
    rows = part_ref.shape[0]
    reached = dot(halos_ref[...], in_order(place_ref, halo_ref))
    reached = reached[:TILE] + reached[TILE:]
    image = jnp.concatenate([part_ref[pl.ds(0, rows - TILE), :], part_ref[pl.ds(rows - TILE, TILE), :] + reached], axis=0)
    image = image * factors_ref[2 * degree][:1]
    if degree > 0:
        image = image - factors_ref[2 * degree + 1][:1] * before_ref[...]
    return image


def first_kernel(
    place_ref, count_ref, factors_ref, old_ref, halo_ref, halos_ref, states_ref, high_ref, low_ref, own_ref, cross_ref,
    fields_ref, part_ref, outgoing_ref, start_ref, base_ref
):
    live = lax.broadcasted_iota(jnp.int32, states_ref.shape, 0) < count_ref[0]
    start_ref[...] = jnp.where(live, states_ref[...], 0.0)
    fields_ref[...] = jnp.where(live, updated(0, place_ref, factors_ref, old_ref, halo_ref, halos_ref, None), 0.0)
    local_part(fields_ref[...], high_ref, low_ref, own_ref, part_ref, outgoing_ref)
    base_ref[...] = selected(
        cross_ref, part_ref[...] * factors_ref[2][:1] - factors_ref[3][:1] * start_ref[...]
    )


def second_kernel(
    place_ref, factors_ref, old_ref, halo_ref, halos_ref, start_ref, high_ref, low_ref, own_ref,
    fields_ref, part_ref, outgoing_ref
):
    fields_ref[...] = updated(1, place_ref, factors_ref, old_ref, halo_ref, halos_ref, start_ref)
    local_part(fields_ref[...], high_ref, low_ref, own_ref, part_ref, outgoing_ref)


def last_kernel(place_ref, factors_ref, part_ref, halo_ref, halos_ref, before_ref, fields_ref, copies_ref):
    fields_ref[...] = updated(2, place_ref, factors_ref, part_ref, halo_ref, halos_ref, before_ref)
    for copy in range(copies_ref.shape[0]):
        copies_ref[copy] = fields_ref[...].astype(BF16)


def end_kernel(scaling, fields_ref, summed_ref, filtered_ref, margin_ref):
    filtered_ref[...] = fields_ref[...]
    margin_ref[...] = summed_ref[...] * scaling


def margin_kernel(band_ref, every_ref, partial_ref):
    bands, _, width = every_ref.shape
    wanted = 2 * bands
    order = [band % 2 * (bands // 2) + band // 2 for band in range(bands)]
    row = lax.broadcasted_iota(jnp.int32, (wanted, width), 0)
    column = lax.broadcasted_iota(jnp.int32, (wanted, width), 1)
    target = (bands - 1 - jnp.right_shift(row, 1)) * wanted + 2 * band_ref[0] + jnp.bitwise_and(row, 1)
    pick = jnp.where(column == target, 1.0, 0.0).astype(BF16)
    chosen = [
        lax.dot_general(pick, every_ref[order[band]], (((1,), (1,)), ((), ())), preferred_element_type=F32).astype(BF16)
        for band in reversed(range(bands))
    ]
    chosen = jnp.concatenate(chosen, axis=0)
    for band in range(0, bands, 2):
        both = jnp.concatenate([every_ref[order[band]], every_ref[order[band + 1]]], axis=1)
        partial_ref[:, pl.ds(band * width, 2 * width)] = dot(chosen, both).astype(BF16)


def call(kernel, operands, specs, outs, flops, scratch=()):
    moved = sum(x.size * x.dtype.itemsize for x in (*operands, *outs))
    return pl.pallas_call(
        kernel,
        out_shape=tuple(outs),
        in_specs=specs,
        out_specs=tuple(VMEM for _ in outs),
        scratch_shapes=list(scratch),
        compiler_params=pltpu.CompilerParams(vmem_limit_bytes=16 * 1024 * 1024),
        cost_estimate=pl.CostEstimate(flops=flops, bytes_accessed=moved, transcendentals=0),
    )(*operands)


def shape(dims, dtype=F32):
    return jax.ShapeDtypeStruct(dims, dtype)


def across(crossing, parts):
    route = []
    for at in range(parts):
        place = at % GROUP
        if place >= 5 and at + GROUP < parts:
            route.append((at, at + GROUP))
        if place <= 2 and at >= GROUP:
            route.append((at, at - GROUP))
    return lax.ppermute(crossing, "grid", route)


def exchanged(outgoing, relayed, place, parts):
    zeros = jnp.zeros_like(relayed)
    down = jnp.where(place >= 5, relayed, zeros)
    up = jnp.where(place <= 2, relayed, zeros)
    gap = jnp.zeros((outgoing.shape[0] - 2 * relayed.shape[0], relayed.shape[1]), BF16)
    message = (outgoing + jnp.concatenate([down, gap, up], axis=0)).reshape(GROUP, -1, outgoing.shape[1])
    groups = [list(range(first, first + GROUP)) for first in range(0, parts, GROUP)]
    received = lax.all_to_all(message, "grid", 0, 0, axis_index_groups=groups, tiled=True)
    return received


def on_device(states, potential, bounds, point_count, send_rows, stencil_table):
    rows, width = states.shape
    parts = lax.axis_size("grid")
    bands = lax.axis_size("band")
    slots = GROUP * 64
    place = jnp.bitwise_and(lax.axis_index("grid"), GROUP - 1).reshape(1)
    band = lax.axis_index("band").reshape(1)

    rounded, send_rows = lax.optimization_barrier((states.astype(BF16), send_rows))
    sends = send_rows[0].astype(BF16)
    cross, crossing = call(
        begin_kernel,
        (place, band, sends, rounded),
        [SMEM, SMEM, VMEM, VMEM],
        [shape((REACH * 64, rows), BF16), shape((REACH * 64, width), BF16)],
        10_000_000,
    )
    relayed = across(crossing, parts)
    own, high, low, halos, factors, part, outgoing, reach, base = call(
        build_kernel,
        (place, bounds.reshape(1, 3), potential.reshape(1, rows), stencil_table, states, sends, cross),
        [SMEM] + [VMEM] * 6,
        [
            shape((slots, rows), BF16),
            shape((rows, rows), BF16),
            shape((rows, rows), BF16),
            shape((2 * TILE, 2 * REACH * 64), BF16),
            shape((2 * DEGREE, 8, TILE)),
            shape((rows, width)),
            shape((slots, width), BF16),
            shape((2 * REACH * 64, 2 * REACH * 64), BF16),
            shape((REACH * 64, width)),
        ],
        50_000_000,
    )
    square = shape((rows, width))
    outs = [square, square, shape((slots, width), BF16)]

    def crossed(degree, base, halo):
        (crossing,) = call(
            functools.partial(crossing_kernel, degree),
            (place, factors, base, halo, reach),
            [SMEM] + [VMEM] * 4,
            [shape((REACH * 64, width), BF16)],
            40_000_000,
        )
        return across(crossing, parts)

    halo = exchanged(outgoing, relayed, place[0], parts)
    relayed = crossed(0, base, halo)
    first, part, outgoing, start, base = call(
        first_kernel,
        (place, point_count, factors, part, halo, halos, states, high, low, own, cross),
        [SMEM, SMEM] + [VMEM] * 9,
        outs + [square, shape((REACH * 64, width))],
        80_000_000,
    )
    halo = exchanged(outgoing, relayed, place[0], parts)
    relayed = crossed(1, base, halo)
    second, part, outgoing = call(
        second_kernel,
        (place, factors, part, halo, halos, start, high, low, own),
        [SMEM] + [VMEM] * 8,
        outs,
        80_000_000,
    )
    halo = exchanged(outgoing, relayed, place[0], parts)
    fields, extra = call(
        last_kernel,
        (place, factors, part, halo, halos, first),
        [SMEM] + [VMEM] * 5,
        [square, shape((bands // 2, rows, width), BF16)],
        40_000_000,
    )
    alike = [list(range(core, bands, 2)) for core in range(2)]
    chips = [[first, first + 1] for first in range(0, bands, 2)]
    alike_bands = lax.all_to_all(extra, "band", 0, 0, axis_index_groups=alike, tiled=True)
    every_band = lax.all_gather(alike_bands, "band", axis=0, axis_index_groups=chips, tiled=True)
    (partial_sums,) = call(
        margin_kernel,
        (band, every_band),
        [SMEM, VMEM],
        [shape((2 * parts, bands * width), BF16)],
        80_000_000,
    )
    blocks = lax.all_to_all(
        partial_sums.reshape(parts, 2, bands * width),
        "grid",
        0,
        0,
        axis_index_groups=[list(reversed(range(parts)))],
        tiled=True,
    )
    summed = jnp.sum(blocks.astype(F32), axis=0)
    return call(
        functools.partial(end_kernel, 1.0 / (parts * rows)),
        (fields, summed),
        [VMEM, VMEM],
        [shape((rows, width)), shape(summed.shape)],
        1000,
    )


def solution(mesh):
    placed = (P("grid", "band"), P("grid"), P(), P("grid"), P("grid", None, None), P(None, "grid"))
    return jax.shard_map(
        on_device,
        mesh=mesh,
        in_specs=placed,
        out_specs=(P("grid", "band"), P(("grid", "band"), None)),
        check_vma=False,
    )
```

```python
import functools

import jax
import jax.numpy as jnp
from jax import lax
from jax.experimental import pallas as pl
from jax.experimental.pallas import tpu as pltpu
from jax.sharding import PartitionSpec as P

SPAN = 6
DEGREE = 3
REACH = 3
GROUP = 8

DIFFERENCE_WEIGHTS = (
    -5369.0 / 1800.0,
    12.0 / 7.0,
    -15.0 / 56.0,
    10.0 / 189.0,
    -1.0 / 112.0,
    2.0 / 1925.0,
    -1.0 / 16632.0,
)
KINETIC_SCALE = 0.5 / 0.49
CENTRE_WEIGHT = -3.0 * KINETIC_SCALE * DIFFERENCE_WEIGHTS[0]
TILE = 128
BF16 = jnp.bfloat16
F32 = jnp.float32
VMEM = pl.BlockSpec(memory_space=pltpu.VMEM)
SMEM = pl.BlockSpec(memory_space=pltpu.SMEM)


def dot(a, b):
    return jnp.dot(a, b, preferred_element_type=F32)


def split(values):
    high = values.astype(BF16)
    return high, (values - high.astype(F32)).astype(BF16)


def select_rows(select_ref, sends_ref, offsets, rows):
    sends = sends_ref[...].astype(F32).astype(jnp.int32)

    def block(offset):
        picks = jnp.full((1, 64), rows, jnp.int32)
        for slot in range(2 * REACH):
            kept = slot - REACH if slot < REACH else slot - REACH + 1
            picks = jnp.where(offset == kept, sends[slot : slot + 1, :], picks)
        return picks

    for pair in range((len(offsets) + 1) // 2):
        two = [block(offset) for offset in offsets[2 * pair : 2 * pair + 2]]
        height = 64 * len(two)
        picks = jnp.concatenate([two[0], two[-1]], axis=1)
        for at in range(0, rows, TILE):
            here = lax.broadcasted_iota(jnp.int32, (TILE, TILE), 0) + at
            hit = jnp.where(here == picks, 1.0, 0.0)
            select_ref[pl.ds(pair * TILE, height), pl.ds(at, TILE)] = jnp.transpose(hit)[:height].astype(BF16)


def begin_kernel(
    place_ref, band_ref, sends_ref, states_ref, own_ref, cross_ref, crossing_ref
):
    place = place_ref[0]
    rows = states_ref.shape[0]
    first = jnp.where(place >= 5, GROUP - place, -REACH - place)
    select_rows(cross_ref, sends_ref, [first + at for at in range(REACH)], rows)
    crossing_ref[...] = dot(cross_ref[...], states_ref[...]).astype(BF16)
    select_rows(own_ref, sends_ref, [at - place for at in range(GROUP)], rows)


def local_part(fields, high_ref, low_ref, own_ref, part_ref, outgoing_ref):
    high, low = split(fields)
    part_ref[...] = dot(high_ref[...], high) + dot(low_ref[...], high) + dot(high_ref[...], low)
    outgoing_ref[...] = dot(own_ref[...], high).astype(BF16)


def build_kernel(
    bounds_ref, potential_ref, table_ref, states_ref, own_ref, cross_ref,
    high_ref, low_ref, halos_ref, factors_ref, part_ref, outgoing_ref, reach_ref, base_ref
):
    rows = states_ref.shape[0]
    stencil = table_ref.shape[0]
    lower, cutoff, upper = (jnp.broadcast_to(bounds_ref[:, at : at + 1], (8, TILE)) for at in range(3))
    half = (upper - cutoff) / 2.0
    middle = (upper + cutoff) / 2.0
    sigma = half / (lower - middle)
    twice = 2.0 / sigma
    factors_ref[0] = sigma / half
    factors_ref[1] = jnp.zeros_like(sigma)
    for degree in range(1, DEGREE):
        following = 1.0 / (twice - sigma)
        factors_ref[2 * degree] = 2.0 * following / half
        factors_ref[2 * degree + 1] = sigma * following
        sigma = following
    middle = middle[:1]
    def gathered(column, row):
        here = lax.broadcasted_iota(jnp.int32, (TILE, TILE), 0) + column
        total = jnp.zeros((TILE, TILE), F32)
        for neighbour in range(stencil):
            weight = -KINETIC_SCALE * DIFFERENCE_WEIGHTS[neighbour % SPAN + 1]
            names = table_ref[neighbour : neighbour + 1, row : row + TILE]
            total = total + jnp.where(here == names, weight, 0.0)
        return total, here

    for row in range(0, rows, TILE):
        diagonal = potential_ref[:, row : row + TILE] + (CENTRE_WEIGHT - middle)

        @pl.loop(0, rows // TILE)
        def _(block, row=row, diagonal=diagonal):
            column = pl.multiple_of(block * TILE, TILE)
            total, here = gathered(column, row)
            right = lax.broadcasted_iota(jnp.int32, (TILE, TILE), 1) + row
            total = total + jnp.where(here == right, diagonal, 0.0)
            high, low = split(jnp.transpose(total))
            high_ref[pl.ds(row, TILE), pl.ds(column, TILE)] = high
            low_ref[pl.ds(row, TILE), pl.ds(column, TILE)] = low

    @pl.loop(0, 2 * REACH * 64 // TILE)
    def _(block):
        column = pl.multiple_of(block * TILE, TILE)
        total, _ = gathered(column + rows + 1, rows - TILE)
        high, low = split(jnp.transpose(total))
        halos_ref[pl.ds(0, TILE), pl.ds(column, TILE)] = high
        halos_ref[pl.ds(TILE, TILE), pl.ds(column, TILE)] = low

    local_part(states_ref[...], high_ref, low_ref, own_ref, part_ref, outgoing_ref)
    crossing = cross_ref.shape[0]
    for at in range(2):
        named = dot(cross_ref[:, rows - TILE :], halos_ref[pl.ds(at * TILE, TILE), :])
        reach_ref[pl.ds(at * crossing, crossing), :] = named.astype(BF16)
    base_ref[...] = selected(cross_ref, part_ref[...] * factors_ref[0][:1])


def selected(select_ref, values):
    high, low = split(values)
    return dot(select_ref[...], high) + dot(select_ref[...], low)


def in_order(place_ref, halo_ref):
    blocks = []
    for slot in range(2 * REACH):
        offset = slot - REACH if slot < REACH else slot - REACH + 1
        blocks.append(halo_ref[jnp.bitwise_and(place_ref[0] - offset, GROUP - 1)])
    return jnp.concatenate(blocks, axis=0)


def crossing_kernel(degree, place_ref, factors_ref, base_ref, halo_ref, reach_ref, crossing_ref):
    rows = crossing_ref.shape[0]
    reached = dot(reach_ref[...], in_order(place_ref, halo_ref))
    reached = (reached[:rows] + reached[rows:]) * factors_ref[2 * degree][:1]
    crossing_ref[...] = (base_ref[...] + reached).astype(BF16)


def updated(degree, place_ref, factors_ref, part_ref, halo_ref, halos_ref, before_ref):
    rows = part_ref.shape[0]
    reached = dot(halos_ref[...], in_order(place_ref, halo_ref))
    reached = reached[:TILE] + reached[TILE:]
    image = jnp.concatenate([part_ref[pl.ds(0, rows - TILE), :], part_ref[pl.ds(rows - TILE, TILE), :] + reached], axis=0)
    image = image * factors_ref[2 * degree][:1]
    if degree > 0:
        image = image - factors_ref[2 * degree + 1][:1] * before_ref[...]
    return image


def first_kernel(
    place_ref, count_ref, factors_ref, old_ref, halo_ref, halos_ref, states_ref, high_ref, low_ref, own_ref, cross_ref,
    fields_ref, part_ref, outgoing_ref, start_ref, base_ref
):
    live = lax.broadcasted_iota(jnp.int32, states_ref.shape, 0) < count_ref[0]
    start_ref[...] = jnp.where(live, states_ref[...], 0.0)
    fields_ref[...] = jnp.where(live, updated(0, place_ref, factors_ref, old_ref, halo_ref, halos_ref, None), 0.0)
    local_part(fields_ref[...], high_ref, low_ref, own_ref, part_ref, outgoing_ref)
    base_ref[...] = selected(
        cross_ref, part_ref[...] * factors_ref[2][:1] - factors_ref[3][:1] * start_ref[...]
    )


def second_kernel(
    place_ref, factors_ref, old_ref, halo_ref, halos_ref, start_ref, high_ref, low_ref, own_ref,
    fields_ref, part_ref, outgoing_ref
):
    fields_ref[...] = updated(1, place_ref, factors_ref, old_ref, halo_ref, halos_ref, start_ref)
    local_part(fields_ref[...], high_ref, low_ref, own_ref, part_ref, outgoing_ref)


def last_kernel(place_ref, factors_ref, part_ref, halo_ref, halos_ref, before_ref, fields_ref, copies_ref):
    fields_ref[...] = updated(2, place_ref, factors_ref, part_ref, halo_ref, halos_ref, before_ref)
    for copy in range(copies_ref.shape[0]):
        copies_ref[copy] = fields_ref[...].astype(BF16)


def end_kernel(scaling, fields_ref, summed_ref, filtered_ref, margin_ref):
    filtered_ref[...] = fields_ref[...]
    margin_ref[...] = summed_ref[...] * scaling


def margin_kernel(band_ref, every_ref, partial_ref):
    bands, _, width = every_ref.shape
    wanted = 2 * bands
    order = [band % 2 * (bands // 2) + band // 2 for band in range(bands)]
    row = lax.broadcasted_iota(jnp.int32, (wanted, width), 0)
    column = lax.broadcasted_iota(jnp.int32, (wanted, width), 1)
    target = (bands - 1 - jnp.right_shift(row, 1)) * wanted + 2 * band_ref[0] + jnp.bitwise_and(row, 1)
    pick = jnp.where(column == target, 1.0, 0.0).astype(BF16)
    chosen = [
        lax.dot_general(pick, every_ref[order[band]], (((1,), (1,)), ((), ())), preferred_element_type=F32).astype(BF16)
        for band in reversed(range(bands))
    ]
    chosen = jnp.concatenate(chosen, axis=0)
    for band in range(0, bands, 2):
        both = jnp.concatenate([every_ref[order[band]], every_ref[order[band + 1]]], axis=1)
        partial_ref[:, pl.ds(band * width, 2 * width)] = dot(chosen, both).astype(BF16)


def call(kernel, operands, specs, outs, flops, scratch=()):
    moved = sum(x.size * x.dtype.itemsize for x in (*operands, *outs))
    return pl.pallas_call(
        kernel,
        out_shape=tuple(outs),
        in_specs=specs,
        out_specs=tuple(VMEM for _ in outs),
        scratch_shapes=list(scratch),
        compiler_params=pltpu.CompilerParams(vmem_limit_bytes=16 * 1024 * 1024),
        cost_estimate=pl.CostEstimate(flops=flops, bytes_accessed=moved, transcendentals=0),
    )(*operands)


def shape(dims, dtype=F32):
    return jax.ShapeDtypeStruct(dims, dtype)


def across(crossing, parts):
    route = []
    for at in range(parts):
        place = at % GROUP
        if place >= 5 and at + GROUP < parts:
            route.append((at, at + GROUP))
        if place <= 2 and at >= GROUP:
            route.append((at, at - GROUP))
    return lax.ppermute(crossing, "grid", route)


def exchanged(outgoing, relayed, place, parts):
    size = relayed.shape[0]
    gap = outgoing.shape[0] - size
    down = jnp.pad(jnp.where(place >= 5, relayed, jnp.zeros_like(relayed)), ((0, gap), (0, 0)))
    up = jnp.pad(jnp.where(place <= 2, relayed, jnp.zeros_like(relayed)), ((gap, 0), (0, 0)))
    message = (outgoing + down + up).reshape(GROUP, -1, outgoing.shape[1])
    groups = [list(range(first, first + GROUP)) for first in range(0, parts, GROUP)]
    received = lax.all_to_all(message, "grid", 0, 0, axis_index_groups=groups, tiled=True)
    return received


def on_device(states, potential, bounds, point_count, send_rows, stencil_table):
    rows, width = states.shape
    parts = lax.axis_size("grid")
    bands = lax.axis_size("band")
    slots = GROUP * 64
    place = jnp.bitwise_and(lax.axis_index("grid"), GROUP - 1).reshape(1)
    band = lax.axis_index("band").reshape(1)

    rounded, send_rows = lax.optimization_barrier((states.astype(BF16), send_rows))
    own, cross, crossing = call(
        begin_kernel,
        (place, band, send_rows[0].astype(BF16), rounded),
        [SMEM, SMEM, VMEM, VMEM],
        [shape((slots, rows), BF16), shape((REACH * 64, rows), BF16), shape((REACH * 64, width), BF16)],
        10_000_000,
    )
    relayed = across(crossing, parts)
    high, low, halos, factors, part, outgoing, reach, base = call(
        build_kernel,
        (bounds.reshape(1, 3), potential.reshape(1, rows), stencil_table, states, own, cross),
        [VMEM] * 6,
        [
            shape((rows, rows), BF16),
            shape((rows, rows), BF16),
            shape((2 * TILE, 2 * REACH * 64), BF16),
            shape((2 * DEGREE, 8, TILE)),
            shape((rows, width)),
            shape((slots, width), BF16),
            shape((2 * REACH * 64, 2 * REACH * 64), BF16),
            shape((REACH * 64, width)),
        ],
        50_000_000,
    )
    square = shape((rows, width))
    outs = [square, square, shape((slots, width), BF16)]

    def crossed(degree, base, halo):
        (crossing,) = call(
            functools.partial(crossing_kernel, degree),
            (place, factors, base, halo, reach),
            [SMEM] + [VMEM] * 4,
            [shape((REACH * 64, width), BF16)],
            40_000_000,
        )
        return across(crossing, parts)

    halo = exchanged(outgoing, relayed, place[0], parts)
    relayed = crossed(0, base, halo)
    first, part, outgoing, start, base = call(
        first_kernel,
        (place, point_count, factors, part, halo, halos, states, high, low, own, cross),
        [SMEM, SMEM] + [VMEM] * 9,
        outs + [square, shape((REACH * 64, width))],
        80_000_000,
    )
    halo = exchanged(outgoing, relayed, place[0], parts)
    relayed = crossed(1, base, halo)
    second, part, outgoing = call(
        second_kernel,
        (place, factors, part, halo, halos, start, high, low, own),
        [SMEM] + [VMEM] * 8,
        outs,
        80_000_000,
    )
    halo = exchanged(outgoing, relayed, place[0], parts)
    fields, extra = call(
        last_kernel,
        (place, factors, part, halo, halos, first),
        [SMEM] + [VMEM] * 5,
        [square, shape((bands // 2, rows, width), BF16)],
        40_000_000,
    )
    alike = [list(range(core, bands, 2)) for core in range(2)]
    chips = [[first, first + 1] for first in range(0, bands, 2)]
    alike_bands = lax.all_to_all(extra, "band", 0, 0, axis_index_groups=alike, tiled=True)
    every_band = lax.all_gather(alike_bands, "band", axis=0, axis_index_groups=chips, tiled=True)
    (partial_sums,) = call(
        margin_kernel,
        (band, every_band),
        [SMEM, VMEM],
        [shape((2 * parts, bands * width), BF16)],
        80_000_000,
    )
    blocks = lax.all_to_all(
        partial_sums.reshape(parts, 2, bands * width),
        "grid",
        0,
        0,
        axis_index_groups=[list(reversed(range(parts)))],
        tiled=True,
    )
    summed = jnp.sum(blocks.astype(F32), axis=0)
    return call(
        functools.partial(end_kernel, 1.0 / (parts * rows)),
        (fields, summed),
        [VMEM, VMEM],
        [shape((rows, width)), shape(summed.shape)],
        1000,
    )


def solution(mesh):
    placed = (P("grid", "band"), P("grid"), P(), P("grid"), P("grid", None, None), P(None, "grid"))
    return jax.shard_map(
        on_device,
        mesh=mesh,
        in_specs=placed,
        out_specs=(P("grid", "band"), P(("grid", "band"), None)),
        check_vma=False,
    )
```
